128 devices in a mesh: gx: 8 (over z, core), gy: 16 (over x, y).
Axes of the slice: x: 4, y: 4, z: 4, core: 2. Of those that a mesh axis runs over, the one named last changes fastest.
Arguments:
- prolong: bfloat16 [8192, 24, 128], P(('gx', 'gy')), may hold values from -0.5 to 0.5
- stiffness: bfloat16 [16384, 4, 128, 128], P(('gx', 'gy')), may hold values from -6 to 6
- request: int32 [16384], P(('gx', 'gy')), may hold values from 0 to 63, as said below
- col_slot: int32 [16384, 4], P(('gx', 'gy')), may hold values from 0 to 127
- col_pos: int32 [16384, 4], P(('gx', 'gy')), may hold values from 0 to 15, as said below
- coarse_owner: int32 [8192, 1], P(('gx', 'gy')), may hold values from 0 to 127; in each aligned block of 64 rows (0 to 63, 64 to 127, ...) no two rows name the same one
Outputs:
- coarse: float32 [16384, 24, 384], P(('gx', 'gy'))
The draws below stay inside these ranges and needn't reach their ends.
Inputs may be any that keep to these rules, and one draw needn't show every extreme that they name: `request`: on each device, entries k * 1 to (k + 1) * 1 - 1 name distinct aggregates of device k, as local indices there. `col_pos`: the 4 entries of one block row are distinct. `coarse_owner`: among one device's 64 aggregates at most 1 share a coarse owner, and on some devices 1 do.
All inputs are finite; a program needn't handle non-finite values.
Results may differ from the reference program's by a relative error of at most 0.0003.
Values may be sent and summed in bfloat16 or wider, within the bound.
No kernel may reach another device: no remote copies, remote signals or barrier semaphores. Data moves between devices by JAX's collectives and lax.ppermute only.
A program may use at most 128 MiB of HBM per device.

```python
import math
import jax
import jax.numpy as jnp
import numpy as np
from jax import lax

AGG_DEV = 64
DOF = 128
CV = 24
MAXNB = 16
SLOT_DEV = 128
BPS = 4
SEND_MAX = 1
IN_ROWS = 128
NAGG = 8192
SLOTS = 16384
DEVICES = 128


def draw_request(key, part):
    per_peer = SLOT_DEV // DEVICES
    scores = jax.random.randint(key, (DEVICES * DEVICES, AGG_DEV), 0, 1 << 20) * AGG_DEV
    scores = scores + jnp.arange(AGG_DEV, dtype=jnp.int32)[None, :]
    chosen = jnp.argsort(scores, axis=1)[:, :per_peer]
    return chosen.reshape(-1).astype(jnp.int32)


def draw_col_pos(key, part):
    scores = jax.random.randint(key, (DEVICES * SLOT_DEV, MAXNB), 0, 1 << 20) * MAXNB
    scores = scores + jnp.arange(MAXNB, dtype=jnp.int32)[None, :]
    chosen = jnp.argsort(scores, axis=1)[:, :BPS]
    return chosen.astype(jnp.int32)


def touch_ends(values, key, low, high):
    longest = values.shape.index(max(values.shape))
    spots = []
    for shift in (0, 1):
        where = [jax.random.randint(jax.random.fold_in(key, axis), (), 0, length) for axis, length in enumerate(values.shape)]
        where[longest] = (where[longest] + shift) % values.shape[longest]
        spots.append(tuple(where))
    return values.at[spots[0]].set(low).at[spots[1]].set(high)


def level_of(own_key, shape, cuts, low, high):
    def one(position, shards_of):
        draws = jax.random.uniform(jax.random.fold_in(jax.random.fold_in(own_key, 6), position), (shards_of,), jnp.float32, low / len(cuts), high / len(cuts))
        return jnp.repeat(jnp.exp(draws), shape[position] // shards_of).reshape((-1,) + (1,) * (len(shape) - position - 1))

    factor_of = one(*cuts[0])
    for cut in cuts[1:]:
        factor_of = factor_of * one(*cut)
    return factor_of


def deal_out(stream_key, own, number, rows, count, top, reach, lean):
    order = jax.random.permutation(stream_key, count)
    heavy_load, common = load_shares(count, rows * top, reach, lean, True), load_shares(count, rows * top, reach, lean, False)
    places = jnp.arange(count)

    def named(sizes, offset_by):
        used = int((sizes > 0).sum())
        fixed = max(1, used // 4)
        shifted = fixed + (places - fixed + offset_by * (used - fixed)) % max(1, count - fixed)
        return jnp.zeros((count,), jnp.int32).at[order[jnp.where(places < fixed, places, shifted)]].set(jnp.asarray(sizes, jnp.int32))

    sizes = jnp.where(number % 4 == 0, named(heavy_load, number // 4), named(common, number - number // 4 - 1))
    mixed = jax.random.permutation(jax.random.fold_in(own, 3), count)
    source_of, taker = mixed[0:count // 2 * 2:2], mixed[1:count // 2 * 2:2]
    room = jnp.minimum(sizes[source_of] - 1, reach - sizes[taker]) // 2
    room = jnp.where((source_of == order[0]) | (taker == order[0]) | (sizes[taker] == 0), 0, jnp.maximum(room, 0))
    shifted = jax.random.randint(jax.random.fold_in(own, 4), (count // 2,), 0, 1 << 20) % (room + 1)
    sizes = sizes.at[source_of].add(-shifted).at[taker].add(shifted)
    items = jnp.searchsorted(jnp.cumsum(sizes), jnp.arange(rows * top), side="right").astype(jnp.int32)
    listing = items.reshape(top, rows).T
    listing = listing[jax.random.permutation(jax.random.fold_in(own, 1), rows)]
    offset_by = jax.random.randint(jax.random.fold_in(own, 2), (rows, 1), 0, top)
    return jnp.take_along_axis(listing, (jnp.arange(top)[None, :] + offset_by) % top, axis=1)


def load_shares(count, total, reach, slope, full):
    portions = [(1 << 20) // math.isqrt(rank ** slope) + 1 for rank in range(1, count + 1)]
    largest = reach if full else min(reach, max(-(-total // count), total * portions[0] // sum(portions)))
    least = 1 if total - largest >= count - 1 else 0
    holding, rest = [largest] + [least] * (count - 1), total - largest - least * (count - 1)
    while rest > 0:
        candidates = [i for i in range(1, count) if holding[i] < largest] or [i for i in range(1, count) if holding[i] < reach]
        whole, budget = sum([portions[i] for i in candidates]), rest
        for i in candidates:
            addition = min(reach - holding[i], max(1, budget * portions[i] // whole), rest)
            holding[i] = holding[i] + addition
            rest = rest - addition
    return np.array(holding)


def bell_draw(own_key, extent, width, limit, shards=(), held_as=jnp.bfloat16):
    values = width * jax.random.normal(own_key, extent, jnp.float32)
    if shards:
        values = values * level_of(own_key, extent, shards, -0.22, 0.18)
    return jnp.clip(values, -limit, limit).astype(held_as)


def setup_inputs(seed: int = 0) -> dict:
    arg_keys = jax.random.split(jax.random.key(seed), 7)
    prolong = bell_draw(arg_keys[0], (NAGG, CV, DOF), DOF ** -0.5, 0.5, ((0, 128),))
    stiffness = bell_draw(arg_keys[1], (SLOTS, BPS, DOF, DOF), 1.0, 6.0, ((0, 128),))
    request = draw_request(jax.random.fold_in(arg_keys[6], 71), 0)
    col_slot = touch_ends(jax.random.randint(arg_keys[3], (SLOTS, BPS), 0, SLOT_DEV), jax.random.fold_in(arg_keys[3], 1), 0, SLOT_DEV - 1).astype(jnp.int32)
    col_pos = draw_col_pos(jax.random.fold_in(arg_keys[6], 71), 0)
    coarse_owner_keys = jax.random.split(jax.random.fold_in(arg_keys[5], 1), NAGG // AGG_DEV)
    coarse_owner_turns = jax.random.permutation(jax.random.fold_in(arg_keys[5], 3), NAGG // AGG_DEV)
    coarse_owner = jax.vmap(lambda own, number: deal_out(jax.random.fold_in(arg_keys[5], 2), own, number, AGG_DEV, DEVICES, 1, SEND_MAX, 2))(coarse_owner_keys, coarse_owner_turns).reshape((NAGG, 1))
    return {"prolong": prolong, "stiffness": stiffness, "request": request, "col_slot": col_slot, "col_pos": col_pos, "coarse_owner": coarse_owner}


HIGH = lax.Precision.HIGHEST


def device_rows(prolong, stiff_block, request_block, slot_block, pos_block):
    per_peer = SLOT_DEV // DEVICES
    gid = (jnp.arange(SLOT_DEV, dtype=jnp.int32) // per_peer) * AGG_DEV + request_block.astype(jnp.int32)
    fetched = prolong[gid].astype(jnp.float32)
    col_rows = fetched[slot_block]
    applied = jnp.einsum("tqij,tqej->tqei", stiff_block.astype(jnp.float32), col_rows, precision=HIGH)
    partial_value = jnp.einsum("tci,tqei->tqce", fetched, applied, precision=HIGH)
    column_hot = (pos_block[:, :, None] == jnp.arange(MAXNB, dtype=jnp.int32)[None, None, :]).astype(jnp.float32)
    spread = jnp.einsum("tqce,tqn->tcne", partial_value, column_hot, precision=HIGH)
    return gid, spread.reshape(SLOT_DEV, CV, MAXNB * CV)


def reference(prolong, stiffness, request, col_slot, col_pos, coarse_owner):
    stiff_dev = stiffness.reshape(DEVICES, SLOT_DEV, BPS, DOF, DOF)
    request_dev = request.reshape(DEVICES, SLOT_DEV)
    slot_dev = col_slot.reshape(DEVICES, SLOT_DEV, BPS)
    pos_dev = col_pos.reshape(DEVICES, SLOT_DEV, BPS)

    def accumulate(total, pieces):
        gid, spread = device_rows(prolong, pieces[0], pieces[1], pieces[2], pieces[3])
        return total.at[gid].add(spread), None

    start = jnp.zeros((NAGG, CV, MAXNB * CV), jnp.float32)
    fine_coarse, _ = lax.scan(accumulate, start, (stiff_dev, request_dev, slot_dev, pos_dev))
    owners = coarse_owner[:, 0].reshape(DEVICES, AGG_DEV)
    peer_ids = jnp.arange(DEVICES, dtype=jnp.int32)
    owner_one = (owners[:, :, None] == peer_ids[None, None, :]).astype(jnp.int32)
    before = jnp.cumsum(owner_one, axis=1) - owner_one
    row_rank = jnp.sum(before * owner_one, axis=2)
    source = jnp.arange(DEVICES, dtype=jnp.int32)[:, None]
    target = (owners * IN_ROWS + source * SEND_MAX + row_rank).reshape(-1).astype(jnp.int32)
    coarse = jnp.zeros((DEVICES * IN_ROWS, CV, MAXNB * CV), jnp.float32).at[target].set(fine_coarse)
    return coarse
```

```python
import jax
import jax.numpy as jnp
from jax import lax
from jax.experimental import pallas as pl
from jax.experimental.pallas import tpu as pltpu
from jax.sharding import PartitionSpec as P

MAXNB = 16
AXES = ("gx", "gy")
F32 = jnp.float32
BF16 = jnp.bfloat16
I16 = jnp.int16
I32 = jnp.int32

TOP = 32766.0
TINY = 2.0**-120
LANES = 128
SUB = 32


def lane_ids(rows):
    return lax.broadcasted_iota(I32, (rows, LANES), 1)


def exponent(rows):
    top = jnp.maximum(jnp.max(jnp.abs(rows), axis=1, keepdims=True), TINY)
    return jnp.ceil(jnp.log2(top))


def gather_kernel(asked, prolong, out):
    def step(d, carry):
        out[d] = prolong[asked[d, 0, 0]]
        return carry

    lax.fori_loop(0, out.shape[0], step, 0, unroll=8)


def partial_kernel(slot, fetched, stiff, out, padded):
    block = stiff.shape[0]
    rows = fetched.shape[1]
    first = pl.program_id(0) * block
    per_row = stiff.shape[1]

    @pl.when(pl.program_id(0) == 0)
    def _():
        def fill(t, carry):
            padded[t, 0:rows, :] = fetched[t]
            padded[t, rows:SUB, :] = jnp.zeros((SUB - rows, LANES), BF16)
            return carry

        lax.fori_loop(0, fetched.shape[0], fill, 0, unroll=8)

    lanes = lane_ids(rows)
    for i in range(block):
        t = first + i
        mine = padded[t]
        stack = []
        for q in range(0, per_row, 2):
            pair = jnp.concatenate([stiff[i, q], stiff[i, q + 1]], axis=1)
            both = jnp.dot(mine, pair, preferred_element_type=F32)
            for h in range(2):
                w = both[0:rows, h * LANES : (h + 1) * LANES]
                high = w.astype(BF16).astype(F32)
                stack += [high, w - high]
        left = jnp.concatenate(stack, axis=0).astype(BF16)
        right = jnp.concatenate([padded[slot[q, t]] for q in range(per_row)], axis=0)
        prod = lax.dot_general(left, right, (((1,), (1,)), ((), ())), preferred_element_type=F32)
        value = jnp.zeros((rows, LANES), F32)
        for q in range(per_row):
            own = prod[2 * q * rows : (2 * q + 1) * rows] + prod[(2 * q + 1) * rows : (2 * q + 2) * rows]
            value = jnp.where(lanes // SUB == q, own, value)
        e = exponent(value)
        code = jnp.round(value * (jnp.exp2(-e) * TOP))
        code = jnp.where(lanes == rows, e, code)
        out[i] = code.astype(I16)


def place_kernel(asked, owner, blocks, out, acc):
    devices, rows, _ = blocks.shape
    aggs = acc.shape[0]
    tiles = acc.shape[2] // LANES
    lanes = lane_ids(rows)
    lane8 = lane_ids(8)

    def clear(a, carry):
        acc[a] = jnp.zeros(acc.shape[1:], F32)
        return carry

    lax.fori_loop(0, aggs, clear, 0, unroll=4)

    def clear_out(d, carry):
        out[d] = jnp.zeros(out.shape[1:], I16)
        return carry

    lax.fori_loop(0, devices, clear_out, 0, unroll=4)

    def add(d, carry):
        code = blocks[d].astype(F32)
        value = code * (jnp.exp2(code[:, rows : rows + 1]) * (1.0 / TOP))
        sums = [jnp.zeros((rows, LANES), F32) for _ in range(tiles)]
        for q in range(4):
            start = asked[d, 0, 1 + q] * rows
            turned = pltpu.roll(value, (start - q * SUB + LANES) % LANES, 1)
            for m in range(tiles):
                at = lanes + (m * LANES - start)
                sums[m] = jnp.where((at >= 0) & (at < rows), turned, sums[m])
        a = asked[d, 0, 0]
        for m in range(tiles):
            acc[a, :, m * LANES : (m + 1) * LANES] += sums[m]
        return carry

    lax.fori_loop(0, devices, add, 0, unroll=2)

    def send(a, carry):
        parts = []
        scales = jnp.zeros((8, LANES), F32)
        for m in range(tiles):
            value = acc[a, :, m * LANES : (m + 1) * LANES]
            e = exponent(value)
            parts.append(jnp.round(value * (jnp.exp2(-e) * TOP)))
            for r in range(rows // 8):
                scales = jnp.where(lane8 == m * (rows // 8) + r, e[8 * r : 8 * r + 8], scales)
        out[owner[0, a]] = jnp.concatenate(parts + [scales], axis=0).astype(I16)
        return carry

    lax.fori_loop(0, aggs, send, 0, unroll=2)


def decode_kernel(code, out):
    rows = out.shape[1]
    tiles = out.shape[2] // LANES
    bands = rows // 8
    for j in range(code.shape[0]):
        x = code[j].astype(F32)
        scales = jnp.exp2(x[rows * tiles : rows * tiles + 8]) * (1.0 / TOP)
        for m in range(tiles):
            for r in range(bands):
                i = m * bands + r
                out[j, 8 * r : 8 * r + 8, m * LANES : (m + 1) * LANES] = (
                    x[8 * i : 8 * i + 8] * scales[:, i : i + 1]
                )


def swap(x):
    return lax.all_to_all(x, AXES, split_axis=0, concat_axis=0, tiled=True)


def per_device(prolong, stiffness, request, col_slot, col_pos, coarse_owner):
    devices = lax.axis_size(AXES)
    aggs, rows, dof = prolong.shape
    per_row = stiffness.shape[1]
    width = MAXNB * rows
    smem = pl.BlockSpec(memory_space=pltpu.SMEM)

    asking = jnp.concatenate([request[:, None], col_pos], axis=1)[:, None, :]
    asked = swap(asking)

    picked = pl.pallas_call(
        gather_kernel,
        out_shape=jax.ShapeDtypeStruct((devices, rows, dof), BF16),
        in_specs=[smem, pl.BlockSpec(memory_space=pltpu.VMEM)],
        out_specs=pl.BlockSpec(memory_space=pltpu.VMEM),
        name="pick",
    )(asked, prolong)
    fetched = swap(picked)

    block = 8
    sent = pl.pallas_call(
        partial_kernel,
        grid=(devices // block,),
        out_shape=jax.ShapeDtypeStruct((devices, rows, LANES), I16),
        in_specs=[
            smem,
            pl.BlockSpec((devices, rows, dof), lambda g: (0, 0, 0)),
            pl.BlockSpec((block, per_row, dof, dof), lambda g: (g, 0, 0, 0)),
        ],
        out_specs=pl.BlockSpec((block, rows, LANES), lambda g: (g, 0, 0)),
        scratch_shapes=[pltpu.VMEM((devices, SUB, dof), BF16)],
        name="partial",
    )(col_slot.T, fetched, stiffness)
    blocks = swap(sent)

    depth = rows * (width // LANES) + 8
    rows_out = pl.pallas_call(
        place_kernel,
        out_shape=jax.ShapeDtypeStruct((devices, depth, LANES), I16),
        in_specs=[smem, smem, pl.BlockSpec(memory_space=pltpu.VMEM)],
        out_specs=pl.BlockSpec(memory_space=pltpu.VMEM),
        scratch_shapes=[pltpu.VMEM((aggs, rows, width), F32)],
        name="place",
    )(asked, coarse_owner.T, blocks)
    arrived = swap(rows_out)

    step = 16
    return pl.pallas_call(
        decode_kernel,
        grid=(devices // step,),
        out_shape=jax.ShapeDtypeStruct((devices, rows, width), F32),
        in_specs=[pl.BlockSpec((step, depth, LANES), lambda g: (g, 0, 0))],
        out_specs=pl.BlockSpec((step, rows, width), lambda g: (g, 0, 0)),
        name="decode",
    )(arrived)


def solution(mesh):
    placed = (
        P(AXES, None, None),
        P(AXES, None, None, None),
        P(AXES),
        P(AXES, None),
        P(AXES, None),
        P(AXES, None),
    )
    return jax.shard_map(
        per_device, mesh=mesh, in_specs=placed, out_specs=P(AXES, None, None), check_vma=False
    )
```

```python
import jax
import jax.numpy as jnp
from jax import lax
from jax.experimental import pallas as pl
from jax.experimental.pallas import tpu as pltpu
from jax.sharding import PartitionSpec as P

MAXNB = 16
AXES = ("gx", "gy")
F32 = jnp.float32
BF16 = jnp.bfloat16
I16 = jnp.int16
I32 = jnp.int32

TOP = 32766.0
TINY = 2.0**-120
LANES = 128
SUB = 32


def lane_ids(rows):
    return lax.broadcasted_iota(I32, (rows, LANES), 1)


def level(top):
    return jnp.ceil(8.0 * jnp.log2(jnp.maximum(top, TINY)))


def gather_kernel(asked, prolong, out):
    def step(d, carry):
        out[d] = prolong[asked[d, 0, 0]]
        return carry

    lax.fori_loop(0, out.shape[0], step, 0, unroll=16)


def partial_kernel(slot, fetched, stiff, out, padded):
    block = stiff.shape[0]
    rows = fetched.shape[1]
    first = pl.program_id(0) * block
    per_row = stiff.shape[1]

    @pl.when(pl.program_id(0) == 0)
    def _():
        def fill(t, carry):
            padded[t, 0:rows, :] = fetched[t]
            padded[t, rows:SUB, :] = jnp.zeros((SUB - rows, LANES), BF16)
            return carry

        lax.fori_loop(0, fetched.shape[0], fill, 0, unroll=8)

    lanes = lane_ids(rows)
    for i in range(block):
        t = first + i
        mine = padded[t]
        highs = []
        lows = []
        for q in range(0, per_row, 2):
            pair = jnp.concatenate([stiff[i, q], stiff[i, q + 1]], axis=1)
            both = jnp.dot(mine, pair, preferred_element_type=F32)
            for h in range(2):
                w = both[0:rows, h * LANES : (h + 1) * LANES]
                high = w.astype(BF16).astype(F32)
                highs.append(high)
                lows.append(w - high)
        left = jnp.concatenate(
            [jnp.concatenate(highs, axis=0).astype(BF16), jnp.concatenate(lows, axis=0).astype(BF16)], axis=1
        )
        right = jnp.concatenate([padded[slot[q, t]] for q in range(per_row)], axis=0)
        right = jnp.concatenate([right, right], axis=1)
        prod = lax.dot_general(left, right, (((1,), (1,)), ((), ())), preferred_element_type=F32)
        value = prod[0:rows]
        for q in range(1, per_row):
            value = jnp.where(lanes < q * SUB, value, prod[q * rows : (q + 1) * rows])
        e = level(jnp.max(jnp.abs(value), axis=1, keepdims=True))
        code = jnp.round(value * (jnp.exp2(e * -0.125) * TOP))
        code = jnp.where(lanes == rows, e, code)
        out[i] = code.astype(I16)


def place_kernel(asked, owner, blocks, out, acc):
    devices, rows, _ = blocks.shape
    aggs = acc.shape[0]
    tiles = acc.shape[2] // LANES
    lanes = lane_ids(8)
    bands = rows // 8
    sub8 = lax.broadcasted_iota(I32, (8, LANES), 0)

    def clear(a, carry):
        acc[a] = jnp.zeros(acc.shape[1:], F32)
        return carry

    lax.fori_loop(0, aggs, clear, 0, unroll=8)

    def clear_out(d, carry):
        out[d] = jnp.zeros(out.shape[1:], I16)
        return carry

    lax.fori_loop(0, devices, clear_out, 0, unroll=8)

    def add(d, carry):
        code = blocks[d].astype(F32)
        scale = jnp.exp2(code[:, rows : rows + 1] * 0.125) * (1.0 / TOP)
        sums = [jnp.zeros((rows, LANES), F32) for _ in range(tiles)]
        for q in range(4):
            start = asked[d, 0, 1 + q]
            turned = pltpu.roll(code, (start - q * SUB + LANES) & (LANES - 1), 1)
            for m in range(tiles):
                at = (lanes + m * LANES) - start
                inside = at.astype(jnp.uint32) < rows
                inside = jnp.concatenate([inside] * bands, axis=0)
                sums[m] = jnp.where(inside, turned, sums[m])
        a = asked[d, 0, 0]
        for m in range(tiles):
            acc[a, :, m * LANES : (m + 1) * LANES] += sums[m] * scale
        return carry

    lax.fori_loop(0, devices, add, 0, unroll=8)

    def send(a, carry):
        parts = []
        scales = jnp.zeros((8, LANES), F32)
        for m in range(tiles):
            value = acc[a, :, m * LANES : (m + 1) * LANES]
            e = level(jnp.max(jnp.abs(value), axis=0, keepdims=True))
            parts.append(jnp.round(value * (jnp.exp2(e * -0.125) * TOP)))
            scales = jnp.where(sub8 == m, e, scales)
        out[owner[0, a]] = jnp.concatenate(parts + [scales], axis=0).astype(I16)
        return carry

    lax.fori_loop(0, aggs, send, 0, unroll=8)


def decode_kernel(code, out):
    rows = out.shape[1]
    tiles = out.shape[2] // LANES
    for j in range(code.shape[0]):
        x = code[j].astype(F32)
        scales = jnp.exp2(x[rows * tiles : rows * tiles + 8] * 0.125) * (1.0 / TOP)
        for m in range(tiles):
            out[j, :, m * LANES : (m + 1) * LANES] = x[rows * m : rows * (m + 1)] * scales[m : m + 1]


def swap(x):
    return lax.all_to_all(x, AXES, split_axis=0, concat_axis=0, tiled=True)


def per_device(prolong, stiffness, request, col_slot, col_pos, coarse_owner):
    devices = lax.axis_size(AXES)
    aggs, rows, dof = prolong.shape
    per_row = stiffness.shape[1]
    width = MAXNB * rows
    smem = pl.BlockSpec(memory_space=pltpu.SMEM)

    asking = jnp.concatenate([request[:, None], col_pos * rows], axis=1)[:, None, :]
    asked = swap(asking)

    picked = pl.pallas_call(
        gather_kernel,
        out_shape=jax.ShapeDtypeStruct((devices, rows, dof), BF16),
        in_specs=[smem, pl.BlockSpec(memory_space=pltpu.VMEM)],
        out_specs=pl.BlockSpec(memory_space=pltpu.VMEM),
        name="pick",
        compiler_params=pltpu.CompilerParams(vmem_limit_bytes=4 << 20),
    )(asked, prolong)
    fetched = swap(picked)

    block = 32
    sent = pl.pallas_call(
        partial_kernel,
        grid=(devices // block,),
        out_shape=jax.ShapeDtypeStruct((devices, rows, LANES), I16),
        in_specs=[
            smem,
            pl.BlockSpec((devices, rows, dof), lambda g: (0, 0, 0)),
            pl.BlockSpec((block, per_row, dof, dof), lambda g: (g, 0, 0, 0)),
        ],
        out_specs=pl.BlockSpec((block, rows, LANES), lambda g: (g, 0, 0)),
        scratch_shapes=[pltpu.VMEM((devices, SUB, dof), BF16)],
        name="partial",
        compiler_params=pltpu.CompilerParams(vmem_limit_bytes=48 << 20),
    )(col_slot.T, fetched, stiffness)
    blocks = swap(sent)

    depth = rows * (width // LANES) + 8
    rows_out = pl.pallas_call(
        place_kernel,
        out_shape=jax.ShapeDtypeStruct((devices, depth, LANES), I16),
        in_specs=[smem, smem, pl.BlockSpec(memory_space=pltpu.VMEM)],
        out_specs=pl.BlockSpec(memory_space=pltpu.VMEM),
        scratch_shapes=[pltpu.VMEM((aggs, rows, width), F32)],
        name="place",
        compiler_params=pltpu.CompilerParams(vmem_limit_bytes=16 << 20),
    )(asked, coarse_owner.T, blocks)
    arrived = swap(rows_out)

    step = 16
    return pl.pallas_call(
        decode_kernel,
        grid=(devices // step,),
        out_shape=jax.ShapeDtypeStruct((devices, rows, width), F32),
        in_specs=[pl.BlockSpec((step, depth, LANES), lambda g: (g, 0, 0))],
        out_specs=pl.BlockSpec((step, rows, width), lambda g: (g, 0, 0)),
        name="decode",
        compiler_params=pltpu.CompilerParams(vmem_limit_bytes=16 << 20),
    )(arrived)


def solution(mesh):
    placed = (
        P(AXES, None, None),
        P(AXES, None, None, None),
        P(AXES),
        P(AXES, None),
        P(AXES, None),
        P(AXES, None),
    )
    return jax.shard_map(
        per_device, mesh=mesh, in_specs=placed, out_specs=P(AXES, None, None), check_vma=False
    )
```

```python
import jax
import jax.numpy as jnp
from jax import lax
from jax.experimental import pallas as pl
from jax.experimental.pallas import tpu as pltpu
from jax.sharding import PartitionSpec as P

MAXNB = 16
AXES = ("gx", "gy")
F32 = jnp.float32
BF16 = jnp.bfloat16
I16 = jnp.int16
I32 = jnp.int32

TOP = 32766.0
TINY = 2.0**-120
LANES = 128
SUB = 32


def lane_ids(rows):
    return lax.broadcasted_iota(I32, (rows, LANES), 1)


def level(top):
    return jnp.ceil(8.0 * jnp.log2(jnp.maximum(top, TINY)))


def prep_kernel(request, col_pos, prolong, asking, held, sem):
    copy = pltpu.make_async_copy(prolong, held, sem)
    copy.start()
    heads = jnp.concatenate([request[...], col_pos[...], jnp.zeros((3, LANES), I32)], axis=0)
    asking[...] = heads.T
    copy.wait()


def gather_kernel(asked, prolong, out):
    def step(d, carry):
        out[d] = prolong[asked[d, 0, 0]]
        return carry

    lax.fori_loop(0, out.shape[0], step, 0, unroll=16)


def partial_kernel(slot, fetched, stiff, out, padded, terms):
    block = stiff.shape[0]
    rows = fetched.shape[1]
    g = pl.program_id(0)
    last = pl.num_programs(0) - 1
    per_row = stiff.shape[1]
    lanes = lane_ids(rows)

    def left_product(i):
        mine = padded[g * block + i]
        highs = []
        lows = []
        for q in range(0, per_row, 2):
            pair = jnp.concatenate([stiff[i, q], stiff[i, q + 1]], axis=1)
            both = jnp.dot(mine, pair, preferred_element_type=F32)
            for h in range(2):
                w = both[0:rows, h * LANES : (h + 1) * LANES]
                high = w.astype(BF16).astype(F32)
                highs.append(high)
                lows.append(w - high)
        terms[i, :, 0:LANES] = jnp.concatenate(highs, axis=0).astype(BF16)
        terms[i, :, LANES : 2 * LANES] = jnp.concatenate(lows, axis=0).astype(BF16)

    def right_product(i):
        t = (g - 1) * block + i
        right = jnp.concatenate([padded[slot[q, t]] for q in range(per_row)], axis=0)
        right = jnp.concatenate([right, right], axis=1)
        prod = lax.dot_general(terms[i], right, (((1,), (1,)), ((), ())), preferred_element_type=F32)
        value = prod[0:rows]
        for q in range(1, per_row):
            value = jnp.where(lanes < q * SUB, value, prod[q * rows : (q + 1) * rows])
        e = level(jnp.max(jnp.abs(value), axis=1, keepdims=True))
        code = jnp.round(value * (jnp.exp2(e * -0.125) * TOP))
        code = jnp.where(lanes == rows, e, code)
        out[i] = code.astype(I16)

    @pl.when(g == 0)
    def _():
        def fill(t, carry):
            padded[t, 0:rows, :] = fetched[t]
            padded[t, rows:SUB, :] = jnp.zeros((SUB - rows, LANES), BF16)
            return carry

        lax.fori_loop(0, fetched.shape[0], fill, 0, unroll=8)
        for i in range(block):
            left_product(i)

    @pl.when((g > 0) & (g < last))
    def _():
        for i in range(block):
            right_product(i)
            left_product(i)

    @pl.when(g == last)
    def _():
        for i in range(block):
            right_product(i)


def place_kernel(asked, owner, blocks, out, acc):
    devices, rows, _ = blocks.shape
    aggs = acc.shape[0]
    tiles = acc.shape[2] // LANES
    lanes = lane_ids(8)
    bands = rows // 8
    sub8 = lax.broadcasted_iota(I32, (8, LANES), 0)

    def clear(a, carry):
        acc[a] = jnp.zeros(acc.shape[1:], F32)
        return carry

    lax.fori_loop(0, aggs, clear, 0, unroll=8)

    def clear_out(d, carry):
        out[d] = jnp.zeros(out.shape[1:], I16)
        return carry

    lax.fori_loop(0, devices, clear_out, 0, unroll=8)

    def add(d, carry):
        code = blocks[d].astype(F32)
        scale = jnp.exp2(code[:, rows : rows + 1] * 0.125) * (1.0 / TOP)
        sums = [jnp.zeros((rows, LANES), F32) for _ in range(tiles)]
        for q in range(4):
            start = asked[d, 0, 1 + q] * rows
            turned = pltpu.roll(code, (start - q * SUB + LANES) & (LANES - 1), 1)
            for m in range(tiles):
                at = (lanes + m * LANES) - start
                inside = at.astype(jnp.uint32) < rows
                inside = jnp.concatenate([inside] * bands, axis=0)
                sums[m] = jnp.where(inside, turned, sums[m])
        a = asked[d, 0, 0]
        for m in range(tiles):
            acc[a, :, m * LANES : (m + 1) * LANES] += sums[m] * scale
        return carry

    lax.fori_loop(0, devices, add, 0, unroll=8)

    def send(a, carry):
        parts = []
        scales = jnp.zeros((8, LANES), F32)
        for m in range(tiles):
            value = acc[a, :, m * LANES : (m + 1) * LANES]
            e = level(jnp.max(jnp.abs(value), axis=0, keepdims=True))
            parts.append(jnp.round(value * (jnp.exp2(e * -0.125) * TOP)))
            scales = jnp.where(sub8 == m, e, scales)
        out[owner[0, a]] = jnp.concatenate(parts + [scales], axis=0).astype(I16)
        return carry

    lax.fori_loop(0, aggs, send, 0, unroll=8)


def decode_kernel(code, out):
    rows = out.shape[1]
    tiles = out.shape[2] // LANES
    for j in range(code.shape[0]):
        x = code[j].astype(F32)
        scales = jnp.exp2(x[rows * tiles : rows * tiles + 8] * 0.125) * (1.0 / TOP)
        for m in range(tiles):
            out[j, :, m * LANES : (m + 1) * LANES] = x[rows * m : rows * (m + 1)] * scales[m : m + 1]


def swap(x):
    return lax.all_to_all(x, AXES, split_axis=0, concat_axis=0, tiled=True)


def in_hbm(x):
    return pltpu.with_memory_space_constraint(x, pltpu.HBM)


def per_device(prolong, stiffness, request, col_slot, col_pos, coarse_owner):
    devices = lax.axis_size(AXES)
    aggs, rows, dof = prolong.shape
    per_row = stiffness.shape[1]
    width = MAXNB * rows
    smem = pl.BlockSpec(memory_space=pltpu.SMEM)

    vmem = pl.BlockSpec(memory_space=pltpu.VMEM)
    asking, held = pl.pallas_call(
        prep_kernel,
        out_shape=(
            jax.ShapeDtypeStruct((devices, 8), I32),
            jax.ShapeDtypeStruct((aggs, rows, dof), BF16),
        ),
        in_specs=[vmem, vmem, pl.BlockSpec(memory_space=pltpu.HBM)],
        out_specs=(vmem, vmem),
        scratch_shapes=[pltpu.SemaphoreType.DMA],
        compiler_params=pltpu.CompilerParams(vmem_limit_bytes=4 << 20),
        name="prep",
    )(in_hbm(request[None, :]), in_hbm(col_pos.T), in_hbm(prolong))
    asked = swap(asking[:, None, :])

    picked = pl.pallas_call(
        gather_kernel,
        out_shape=jax.ShapeDtypeStruct((devices, rows, dof), BF16),
        in_specs=[smem, pl.BlockSpec(memory_space=pltpu.VMEM)],
        out_specs=pl.BlockSpec(memory_space=pltpu.VMEM),
        name="pick",
        compiler_params=pltpu.CompilerParams(vmem_limit_bytes=4 << 20),
    )(asked, held)
    fetched = swap(picked)

    block = 16
    steps = devices // block
    sent = pl.pallas_call(
        partial_kernel,
        grid=(steps + 1,),
        out_shape=jax.ShapeDtypeStruct((devices, rows, LANES), I16),
        in_specs=[
            smem,
            pl.BlockSpec((devices, rows, dof), lambda g: (0, 0, 0)),
            pl.BlockSpec((block, per_row, dof, dof), lambda g: (jnp.minimum(g, steps - 1), 0, 0, 0)),
        ],
        out_specs=pl.BlockSpec((block, rows, LANES), lambda g: (jnp.maximum(g - 1, 0), 0, 0)),
        scratch_shapes=[
            pltpu.VMEM((devices, SUB, dof), BF16),
            pltpu.VMEM((block, rows * per_row, 2 * dof), BF16),
        ],
        name="partial",
        compiler_params=pltpu.CompilerParams(vmem_limit_bytes=48 << 20),
    )(in_hbm(col_slot.T), fetched, stiffness)
    blocks = swap(sent)

    depth = rows * (width // LANES) + 8
    rows_out = pl.pallas_call(
        place_kernel,
        out_shape=jax.ShapeDtypeStruct((devices, depth, LANES), I16),
        in_specs=[smem, smem, pl.BlockSpec(memory_space=pltpu.VMEM)],
        out_specs=pl.BlockSpec(memory_space=pltpu.VMEM),
        scratch_shapes=[pltpu.VMEM((aggs, rows, width), F32)],
        name="place",
        compiler_params=pltpu.CompilerParams(vmem_limit_bytes=16 << 20),
    )(asked, in_hbm(coarse_owner.T), blocks)
    arrived = swap(rows_out)

    step = 32
    return pl.pallas_call(
        decode_kernel,
        grid=(devices // step,),
        out_shape=jax.ShapeDtypeStruct((devices, rows, width), F32),
        in_specs=[pl.BlockSpec((step, depth, LANES), lambda g: (g, 0, 0))],
        out_specs=pl.BlockSpec((step, rows, width), lambda g: (g, 0, 0)),
        name="decode",
        compiler_params=pltpu.CompilerParams(vmem_limit_bytes=16 << 20),
    )(arrived)


def solution(mesh):
    placed = (
        P(AXES, None, None),
        P(AXES, None, None, None),
        P(AXES),
        P(AXES, None),
        P(AXES, None),
        P(AXES, None),
    )
    return jax.shard_map(
        per_device, mesh=mesh, in_specs=placed, out_specs=P(AXES, None, None), check_vma=False
    )
```

```python
import jax
import jax.numpy as jnp
from jax import lax
from jax.experimental import pallas as pl
from jax.experimental.pallas import tpu as pltpu
from jax.sharding import PartitionSpec as P

MAXNB = 16
AXES = ("gx", "gy")
F32 = jnp.float32
BF16 = jnp.bfloat16
I16 = jnp.int16
I32 = jnp.int32

TOP = 32766.0
TINY = 2.0**-120
LANES = 128
SUB = 32


def lane_ids(rows):
    return lax.broadcasted_iota(I32, (rows, LANES), 1)


def level(top):
    return jnp.ceil(8.0 * jnp.log2(jnp.maximum(top, TINY)))


def pick_kernel(asked, prolong, out, heads, held, named, sems):
    load = pltpu.make_async_copy(prolong, held, sems.at[0])
    load.start()
    heads[...] = asked[...].T
    name = pltpu.make_async_copy(heads, named, sems.at[1])
    name.start()
    name.wait()
    load.wait()

    def step(d, carry):
        out[d] = held[named[0, d]]
        return carry

    lax.fori_loop(0, out.shape[0], step, 0, unroll=16)


def partial_kernel(slot, fetched, far, out, padded, stiff, sems):
    devices, rows, _ = fetched.shape
    per_row = stiff.shape[1]
    lanes = lane_ids(rows)
    parts = sems.shape[0]
    block = devices // parts
    copies = [
        pltpu.make_async_copy(far.at[pl.ds(g * block, block)], stiff.at[pl.ds(g * block, block)], sems.at[g])
        for g in range(parts)
    ]
    for copy in copies:
        copy.start()

    def fill(t, carry):
        padded[t, 0:rows, :] = fetched[t]
        padded[t, rows:SUB, :] = jnp.zeros((SUB - rows, LANES), BF16)
        return carry

    lax.fori_loop(0, devices, fill, 0, unroll=8)

    def row(t):
        mine = padded[t]
        highs = []
        lows = []
        for q in range(0, per_row, 2):
            pair = jnp.concatenate([stiff[t, q], stiff[t, q + 1]], axis=1)
            both = jnp.dot(mine, pair, preferred_element_type=F32)
            for h in range(2):
                w = both[0:rows, h * LANES : (h + 1) * LANES]
                high = w.astype(BF16).astype(F32)
                highs.append(high)
                lows.append(w - high)
        left = jnp.concatenate(
            [jnp.concatenate(highs, axis=0).astype(BF16), jnp.concatenate(lows, axis=0).astype(BF16)], axis=1
        )
        right = jnp.concatenate([padded[slot[q, t]] for q in range(per_row)], axis=0)
        right = jnp.concatenate([right, right], axis=1)
        prod = lax.dot_general(left, right, (((1,), (1,)), ((), ())), preferred_element_type=F32)
        value = prod[0:rows]
        for q in range(1, per_row):
            value = jnp.where(lanes < q * SUB, value, prod[q * rows : (q + 1) * rows])
        e = level(jnp.max(jnp.abs(value), axis=1, keepdims=True))
        code = jnp.round(value * (jnp.exp2(e * -0.125) * TOP))
        code = jnp.where(lanes == rows, e, code)
        out[t] = code.astype(I16)

    def step(g, carry):
        rest = pl.ds(g * block, block)
        pltpu.make_async_copy(far.at[rest], stiff.at[rest], sems.at[g]).wait()
        for i in range(block):
            row(g * block + i)
        return carry

    lax.fori_loop(0, parts, step, 0)


def place_kernel(heads, owner, blocks, out, acc):
    devices, rows, _ = blocks.shape
    aggs = acc.shape[0]
    tiles = acc.shape[2] // LANES
    lanes = lane_ids(8)
    bands = rows // 8
    sub8 = lax.broadcasted_iota(I32, (8, LANES), 0)

    def clear(a, carry):
        acc[a] = jnp.zeros(acc.shape[1:], F32)
        return carry

    lax.fori_loop(0, aggs, clear, 0, unroll=8)

    def clear_out(d, carry):
        out[d] = jnp.zeros(out.shape[1:], I16)
        return carry

    lax.fori_loop(0, devices, clear_out, 0, unroll=8)

    def add(d, carry):
        code = blocks[d].astype(F32)
        scale = jnp.exp2(code[:, rows : rows + 1] * 0.125) * (1.0 / TOP)
        sums = [jnp.zeros((rows, LANES), F32) for _ in range(tiles)]
        for q in range(4):
            start = heads[1 + q, d] * rows
            turned = pltpu.roll(code, (start - q * SUB + LANES) & (LANES - 1), 1)
            for m in range(tiles):
                at = (lanes + m * LANES) - start
                inside = at.astype(jnp.uint32) < rows
                inside = jnp.concatenate([inside] * bands, axis=0)
                sums[m] = jnp.where(inside, turned, sums[m])
        a = heads[0, d]
        for m in range(tiles):
            acc[a, :, m * LANES : (m + 1) * LANES] += sums[m] * scale
        return carry

    lax.fori_loop(0, devices, add, 0, unroll=32)

    def send(a, carry):
        parts = []
        scales = jnp.zeros((8, LANES), F32)
        for m in range(tiles):
            value = acc[a, :, m * LANES : (m + 1) * LANES]
            e = level(jnp.max(jnp.abs(value), axis=0, keepdims=True))
            parts.append(jnp.round(value * (jnp.exp2(e * -0.125) * TOP)))
            scales = jnp.where(sub8 == m, e, scales)
        out[owner[0, a]] = jnp.concatenate(parts + [scales], axis=0).astype(I16)
        return carry

    lax.fori_loop(0, aggs, send, 0, unroll=8)


def decode_kernel(code, out):
    rows = out.shape[1]
    tiles = out.shape[2] // LANES
    for j in range(code.shape[0]):
        x = code[j].astype(F32)
        scales = jnp.exp2(x[rows * tiles : rows * tiles + 8] * 0.125) * (1.0 / TOP)
        for m in range(tiles):
            out[j, :, m * LANES : (m + 1) * LANES] = x[rows * m : rows * (m + 1)] * scales[m : m + 1]


def swap(x):
    return lax.all_to_all(x, AXES, split_axis=0, concat_axis=0, tiled=True)


def in_hbm(x):
    return pltpu.with_memory_space_constraint(x, pltpu.HBM)


def grant(mib):
    return pltpu.CompilerParams(vmem_limit_bytes=mib << 20)


def per_device(prolong, stiffness, request, col_slot, col_pos, coarse_owner):
    devices = lax.axis_size(AXES)
    aggs, rows, dof = prolong.shape
    per_row = stiffness.shape[1]
    width = MAXNB * rows
    smem = pl.BlockSpec(memory_space=pltpu.SMEM)
    vmem = pl.BlockSpec(memory_space=pltpu.VMEM)
    hbm = pl.BlockSpec(memory_space=pltpu.HBM)

    asking = jnp.concatenate([request[:, None], col_pos, col_pos[:, 0:3]], axis=1)
    asked = swap(asking[:, None, :])[:, 0, :]

    picked, heads = pl.pallas_call(
        pick_kernel,
        out_shape=(
            jax.ShapeDtypeStruct((devices, rows, dof), BF16),
            jax.ShapeDtypeStruct((8, devices), I32),
        ),
        in_specs=[vmem, hbm],
        out_specs=(vmem, vmem),
        scratch_shapes=[
            pltpu.VMEM((aggs, rows, dof), BF16),
            pltpu.SMEM((8, devices), I32),
            pltpu.SemaphoreType.DMA((2,)),
        ],
        compiler_params=grant(4),
        name="pick",
    )(asked, in_hbm(prolong))
    fetched = swap(picked)

    sent = pl.pallas_call(
        partial_kernel,
        out_shape=jax.ShapeDtypeStruct((devices, rows, LANES), I16),
        in_specs=[smem, vmem, hbm],
        out_specs=vmem,
        scratch_shapes=[
            pltpu.VMEM((devices, SUB, dof), BF16),
            pltpu.VMEM((devices, per_row, dof, dof), BF16),
            pltpu.SemaphoreType.DMA((4,)),
        ],
        compiler_params=grant(40),
        name="partial",
    )(in_hbm(col_slot.T), fetched, in_hbm(stiffness))
    blocks = swap(sent)

    depth = rows * (width // LANES) + 8
    rows_out = pl.pallas_call(
        place_kernel,
        out_shape=jax.ShapeDtypeStruct((devices, depth, LANES), I16),
        in_specs=[smem, smem, vmem],
        out_specs=vmem,
        scratch_shapes=[pltpu.VMEM((aggs, rows, width), F32)],
        name="place",
        compiler_params=grant(16),
    )(heads, in_hbm(coarse_owner.T), blocks)
    arrived = swap(rows_out)

    step = 32
    return pl.pallas_call(
        decode_kernel,
        grid=(devices // step,),
        out_shape=jax.ShapeDtypeStruct((devices, rows, width), F32),
        in_specs=[pl.BlockSpec((step, depth, LANES), lambda g: (g, 0, 0))],
        out_specs=pl.BlockSpec((step, rows, width), lambda g: (g, 0, 0)),
        name="decode",
        compiler_params=grant(16),
    )(arrived)


def solution(mesh):
    placed = (
        P(AXES, None, None),
        P(AXES, None, None, None),
        P(AXES),
        P(AXES, None),
        P(AXES, None),
        P(AXES, None),
    )
    return jax.shard_map(
        per_device, mesh=mesh, in_specs=placed, out_specs=P(AXES, None, None), check_vma=False
    )
```

```python
import functools
import math

import jax
import jax.numpy as jnp
from jax import lax
from jax.experimental import pallas as pl
from jax.experimental.pallas import tpu as pltpu
from jax.sharding import PartitionSpec as P

MAXNB = 16
AXES = ("gx", "gy")
F32 = jnp.float32
BF16 = jnp.bfloat16
I16 = jnp.int16
I32 = jnp.int32

TOP = 32766.0
TINY = 2.0**-100
FLOOR = 14
LANES = 128
SUB = 32


def lane_ids(rows):
    return lax.broadcasted_iota(I32, (rows, LANES), 1)


def codes(devices):
    return TOP / (FLOOR + math.log2(devices))


def level(top):
    return jnp.ceil(8.0 * jnp.log2(jnp.maximum(top, TINY)))


def pick_kernel(asked, prolong, out, heads, held, named, sems):
    load = pltpu.make_async_copy(prolong, held, sems.at[0])
    load.start()
    heads[...] = asked[...].T
    name = pltpu.make_async_copy(heads, named, sems.at[1])
    name.start()
    name.wait()
    load.wait()

    def step(d, carry):
        out[d] = held[named[0, d]]
        return carry

    lax.fori_loop(0, out.shape[0], step, 0, unroll=16)


def partial_kernel(slot, fetched, far, out, padded, stiff, sems):
    devices, rows, _ = fetched.shape
    per_row = stiff.shape[1]
    lanes = lane_ids(rows)
    parts = sems.shape[0]
    block = devices // parts
    copies = [
        pltpu.make_async_copy(far.at[pl.ds(g * block, block)], stiff.at[pl.ds(g * block, block)], sems.at[g])
        for g in range(parts)
    ]
    for copy in copies:
        copy.start()

    def fill(t, carry):
        padded[t, 0:rows, :] = fetched[t]
        padded[t, rows:SUB, :] = jnp.zeros((SUB - rows, LANES), BF16)
        return carry

    lax.fori_loop(0, devices, fill, 0, unroll=8)

    def row(t):
        mine = padded[t]
        highs = []
        lows = []
        for q in range(0, per_row, 2):
            pair = jnp.concatenate([stiff[t, q], stiff[t, q + 1]], axis=1)
            both = jnp.dot(mine, pair, preferred_element_type=F32)
            for h in range(2):
                w = both[0:rows, h * LANES : (h + 1) * LANES]
                high = w.astype(BF16).astype(F32)
                highs.append(high)
                lows.append(w - high)
        left = jnp.concatenate(
            [jnp.concatenate(highs, axis=0).astype(BF16), jnp.concatenate(lows, axis=0).astype(BF16)], axis=1
        )
        right = jnp.concatenate([padded[slot[q, t]] for q in range(per_row)], axis=0)
        right = jnp.concatenate([right, right], axis=1)
        prod = lax.dot_general(left, right, (((1,), (1,)), ((), ())), preferred_element_type=F32)
        value = prod[0:rows]
        for q in range(1, per_row):
            value = jnp.where(lanes < q * SUB, value, prod[q * rows : (q + 1) * rows])
        top = jnp.max(jnp.abs(value), axis=1, keepdims=True)
        e = level(top)
        code = jnp.round(value * (jnp.exp2(e * -0.125) * TOP))
        code = jnp.where(lanes == rows, e, code)
        out[t] = code.astype(I16)
        return top

    def step(g, most):
        rest = pl.ds(g * block, block)
        pltpu.make_async_copy(far.at[rest], stiff.at[rest], sems.at[g]).wait()
        for i in range(block):
            most = jnp.maximum(most, row(g * block + i))
        return most

    most = lax.fori_loop(0, parts, step, jnp.zeros((rows, 1), F32))
    most = jnp.broadcast_to(level(jnp.max(most, axis=0, keepdims=True)), (8, LANES)).astype(I16)
    spare = lane_ids(8).astype(I16) == SUB + rows

    def share(t, carry):
        out[t, 0:8, :] = jnp.where(spare, most, out[t, 0:8, :])
        return carry

    lax.fori_loop(0, devices, share, 0, unroll=16)


def place_kernel(heads, owner, blocks, out, unit, acc):
    devices, rows, _ = blocks.shape
    aggs = acc.shape[0]
    tiles = acc.shape[2] // LANES
    lanes = lane_ids(8)
    bands = rows // 8

    def clear(a, carry):
        acc[a] = jnp.zeros(acc.shape[1:], F32)
        return carry

    lax.fori_loop(0, aggs, clear, 0, unroll=8)

    def clear_out(d, carry):
        out[d] = jnp.zeros(out.shape[1:], I16)
        return carry

    lax.fori_loop(0, devices, clear_out, 0, unroll=8)

    def add(d, most):
        code = blocks[d].astype(F32)
        scale = jnp.exp2(code[:, rows : rows + 1] * 0.125) * (1.0 / TOP)
        sums = [jnp.zeros((rows, LANES), F32) for _ in range(tiles)]
        for q in range(4):
            start = heads[1 + q, d] * rows
            turned = pltpu.roll(code, (start - q * SUB + LANES) & (LANES - 1), 1)
            for m in range(tiles):
                at = (lanes + m * LANES) - start
                inside = at.astype(jnp.uint32) < rows
                inside = jnp.concatenate([inside] * bands, axis=0)
                sums[m] = jnp.where(inside, turned, sums[m])
        a = heads[0, d]
        for m in range(tiles):
            acc[a, :, m * LANES : (m + 1) * LANES] += sums[m] * scale
        return jnp.maximum(most, code[0:8])

    most = lax.fori_loop(0, devices, add, jnp.full((8, LANES), -8.0 * 1024, F32), unroll=32)
    most = jnp.broadcast_to(most[0:1, SUB + rows : SUB + rows + 1], (8, LANES))
    unit[...] = most
    inverse = jnp.exp2(FLOOR - most * 0.125)[0:1]
    rate = codes(devices)

    def send(a, carry):
        parts = []
        for m in range(tiles):
            value = acc[a, :, m * LANES : (m + 1) * LANES]
            size = jnp.log2(1.0 + jnp.abs(value) * inverse)
            parts.append(jnp.round(size * jnp.where(value < 0.0, -rate, rate)))
        out[owner[0, a]] = jnp.concatenate(parts, axis=0).astype(I16)
        return carry

    lax.fori_loop(0, aggs, send, 0, unroll=8)


def decode_kernel(devices, unit, code, out):
    rows = out.shape[1]
    tiles = out.shape[2] // LANES
    delta = jnp.exp2(unit[0:1] * 0.125 - FLOOR)
    rate = 1.0 / codes(devices)
    for j in range(code.shape[0]):
        for m in range(tiles):
            x = code[j, rows * m : rows * (m + 1)].astype(F32)
            size = (jnp.exp2(jnp.abs(x) * rate) - 1.0) * jnp.where(x < 0.0, -delta, delta)
            out[j, :, m * LANES : (m + 1) * LANES] = size


def swap(x):
    return lax.all_to_all(x, AXES, split_axis=0, concat_axis=0, tiled=True)


def in_hbm(x):
    return pltpu.with_memory_space_constraint(x, pltpu.HBM)


def grant(mib):
    return pltpu.CompilerParams(vmem_limit_bytes=mib << 20)


def per_device(prolong, stiffness, request, col_slot, col_pos, coarse_owner):
    devices = lax.axis_size(AXES)
    aggs, rows, dof = prolong.shape
    per_row = stiffness.shape[1]
    width = MAXNB * rows
    smem = pl.BlockSpec(memory_space=pltpu.SMEM)
    vmem = pl.BlockSpec(memory_space=pltpu.VMEM)
    hbm = pl.BlockSpec(memory_space=pltpu.HBM)

    asking = jnp.concatenate([request[:, None], col_pos, col_pos[:, 0:3]], axis=1)
    asked = swap(asking[:, None, :])[:, 0, :]

    picked, heads = pl.pallas_call(
        pick_kernel,
        out_shape=(
            jax.ShapeDtypeStruct((devices, rows, dof), BF16),
            jax.ShapeDtypeStruct((8, devices), I32),
        ),
        in_specs=[vmem, hbm],
        out_specs=(vmem, vmem),
        scratch_shapes=[
            pltpu.VMEM((aggs, rows, dof), BF16),
            pltpu.SMEM((8, devices), I32),
            pltpu.SemaphoreType.DMA((2,)),
        ],
        compiler_params=grant(4),
        name="pick",
    )(asked, in_hbm(prolong))
    fetched = swap(picked)

    sent = pl.pallas_call(
        partial_kernel,
        out_shape=jax.ShapeDtypeStruct((devices, rows, LANES), I16),
        in_specs=[smem, vmem, hbm],
        out_specs=vmem,
        scratch_shapes=[
            pltpu.VMEM((devices, SUB, dof), BF16),
            pltpu.VMEM((devices, per_row, dof, dof), BF16),
            pltpu.SemaphoreType.DMA((4,)),
        ],
        compiler_params=grant(40),
        name="partial",
    )(in_hbm(col_slot.T), fetched, in_hbm(stiffness))
    blocks = swap(sent)

    depth = rows * (width // LANES)
    coarse, unit = pl.pallas_call(
        place_kernel,
        out_shape=(
            jax.ShapeDtypeStruct((devices, depth, LANES), I16),
            jax.ShapeDtypeStruct((8, LANES), F32),
        ),
        in_specs=[smem, smem, vmem],
        out_specs=(vmem, vmem),
        scratch_shapes=[pltpu.VMEM((aggs, rows, width), F32)],
        compiler_params=grant(16),
        name="place",
    )(heads, in_hbm(coarse_owner.T), blocks)
    arrived = swap(coarse)

    step = 32
    return pl.pallas_call(
        functools.partial(decode_kernel, devices),
        grid=(devices // step,),
        out_shape=jax.ShapeDtypeStruct((devices, rows, width), F32),
        in_specs=[
            pl.BlockSpec((8, LANES), lambda g: (0, 0)),
            pl.BlockSpec((step, depth, LANES), lambda g: (g, 0, 0)),
        ],
        out_specs=pl.BlockSpec((step, rows, width), lambda g: (g, 0, 0)),
        compiler_params=grant(16),
        name="decode",
    )(unit, arrived)


def solution(mesh):
    placed = (
        P(AXES, None, None),
        P(AXES, None, None, None),
        P(AXES),
        P(AXES, None),
        P(AXES, None),
        P(AXES, None),
    )
    return jax.shard_map(
        per_device, mesh=mesh, in_specs=placed, out_specs=P(AXES, None, None), check_vma=False
    )
```

```python
import math

import jax
import jax.numpy as jnp
from jax import lax
from jax.experimental import pallas as pl
from jax.experimental.pallas import tpu as pltpu
from jax.sharding import PartitionSpec as P

MAXNB = 16
AXES = ("gx", "gy")
F32 = jnp.float32
BF16 = jnp.bfloat16
I16 = jnp.int16
I32 = jnp.int32

TOP = 32766.0
TINY = 2.0**-100
FLOOR = 14
DEPTH = 4
LANES = 128
SUB = 32


def lane_ids(rows):
    return lax.broadcasted_iota(I32, (rows, LANES), 1)


def codes(devices):
    return TOP / (FLOOR + math.log2(devices))


def level(top):
    return jnp.ceil(8.0 * jnp.log2(jnp.maximum(top, TINY)))


def pick_kernel(asked, prolong, far, out, heads, near, held, named, sems):
    load = pltpu.make_async_copy(prolong, held, sems.at[0])
    load.start()
    ways = sems.shape[0] - 2
    size = near.shape[0] // ways
    ahead = [
        pltpu.make_async_copy(far.at[pl.ds(w * size, size)], near.at[pl.ds(w * size, size)], sems.at[2 + w])
        for w in range(ways)
    ]
    for copy in ahead:
        copy.start()
    heads[...] = asked[...].T
    name = pltpu.make_async_copy(heads, named, sems.at[1])
    name.start()
    name.wait()
    load.wait()

    def step(d, carry):
        out[d] = held[named[0, d]]
        return carry

    lax.fori_loop(0, out.shape[0], step, 0, unroll=16)
    for copy in ahead:
        copy.wait()


def partial_kernel(slot, fetched, near, far, out, padded, pairs, stiff, sems):
    devices, rows, dof = fetched.shape
    per_row = stiff.shape[1]
    lanes = lane_ids(rows)
    parts = sems.shape[0]
    block = near.shape[0]
    copies = [
        pltpu.make_async_copy(far.at[pl.ds((g + 1) * block, block)], stiff.at[pl.ds(g * block, block)], sems.at[g])
        for g in range(parts)
    ]
    for copy in copies:
        copy.start()

    def fill(p, carry):
        pairs[p] = jnp.zeros(pairs.shape[1:], BF16)
        for h in range(2):
            mine = fetched[2 * p + h]
            padded[2 * p + h, 0:rows, :] = mine
            padded[2 * p + h, rows:SUB, :] = jnp.zeros((SUB - rows, LANES), BF16)
            pairs[p, SUB * h : SUB * h + rows, LANES * h : LANES * (h + 1)] = mine
        return carry

    lax.fori_loop(0, devices // 2, fill, 0, unroll=4)

    def products(*accs):
        most = jnp.zeros((rows, 1), F32)

        def first(p):
            held, t = (near, 2 * p) if 2 * p < block else (stiff, 2 * p - block)
            for c in range(2):
                tile = jnp.concatenate(
                    [
                        jnp.concatenate([held[t + h, 2 * c], held[t + h, 2 * c + 1]], axis=1)
                        for h in range(2)
                    ],
                    axis=0,
                )
                pltpu.matmul_push_rhs(tile, staging_register=c, mxu_index=0)
                pltpu.matmul_acc_lhs(accs[2 * (p % DEPTH) + c], pairs[p], load_staged_rhs=c)

        def second(p):
            both = [pltpu.matmul_pop(accs[2 * (p % DEPTH) + c]) for c in range(2)]
            lefts = []
            rights = []
            for h in range(2):
                highs = []
                lows = []
                for q in range(per_row):
                    w = both[q // 2][SUB * h : SUB * h + rows, (q % 2) * LANES : (q % 2 + 1) * LANES]
                    high = w.astype(BF16).astype(F32)
                    highs.append(high)
                    lows.append(w - high)
                lefts.append(
                    jnp.concatenate(
                        [jnp.concatenate(highs, axis=0).astype(BF16), jnp.concatenate(lows, axis=0).astype(BF16)],
                        axis=1,
                    )
                )
                rights += [padded[slot[q, 2 * p + h]] for q in range(per_row)]
            right = jnp.concatenate(rights, axis=0)
            right = jnp.concatenate([right, right], axis=1)
            pltpu.matmul_push_rhs(right, staging_register=p % 2, mxu_index=1, transpose=True)
            pltpu.matmul_acc_lhs(accs[2 * DEPTH + p % DEPTH], jnp.concatenate(lefts, axis=0), load_staged_rhs=p % 2)

        def third(p, most):
            prod = pltpu.matmul_pop(accs[2 * DEPTH + p % DEPTH])
            for h in range(2):
                mine = prod[h * per_row * rows : (h + 1) * per_row * rows, h * LANES : (h + 1) * LANES]
                value = mine[0:rows]
                for q in range(1, per_row):
                    value = jnp.where(lanes < q * SUB, value, mine[q * rows : (q + 1) * rows])
                top = jnp.max(jnp.abs(value), axis=1, keepdims=True)
                most = jnp.maximum(most, top)
                e = level(top)
                code = jnp.round(value * (jnp.exp2(e * -0.125) * TOP))
                code = jnp.where(lanes == rows, e, code)
                out[2 * p + h] = code.astype(I16)
            return most

        count = devices // 2
        for i in range(count + 2 * (DEPTH - 1)):
            if 0 < i < count and (2 * i) % block == 0:
                copies[2 * i // block - 1].wait()
            if i < count:
                first(i)
            if 0 <= i - (DEPTH - 1) < count:
                second(i - (DEPTH - 1))
            if 0 <= i - 2 * (DEPTH - 1) < count:
                most = third(i - 2 * (DEPTH - 1), most)

        most = jnp.broadcast_to(level(jnp.max(most, axis=0, keepdims=True)), (8, LANES)).astype(I16)
        spare = lane_ids(8).astype(I16) == SUB + rows

        def share(t, carry):
            out[t, 0:8, :] = jnp.where(spare, most, out[t, 0:8, :])
            return carry

        lax.fori_loop(0, devices, share, 0, unroll=16)

    wide = 2 * LANES
    pl.run_scoped(
        products,
        *[pltpu.ACC(0)((2 * SUB, wide), F32) for _ in range(2 * DEPTH)],
        *[pltpu.ACC(1)((2 * per_row * rows, wide), F32) for _ in range(DEPTH)],
    )


def place_kernel(heads, owner, blocks, out, unit, acc):
    devices, rows, _ = blocks.shape
    aggs = acc.shape[0]
    tiles = acc.shape[2] // LANES
    lanes = lane_ids(8)
    bands = rows // 8

    def clear(a, carry):
        acc[a] = jnp.zeros(acc.shape[1:], F32)
        return carry

    lax.fori_loop(0, aggs, clear, 0, unroll=8)

    def clear_out(d, carry):
        out[d] = jnp.zeros(out.shape[1:], I16)
        return carry

    lax.fori_loop(0, devices, clear_out, 0, unroll=8)

    def add(d, most):
        code = blocks[d].astype(F32)
        scale = jnp.exp2(code[:, rows : rows + 1] * 0.125) * (1.0 / TOP)
        sums = [jnp.zeros((rows, LANES), F32) for _ in range(tiles)]
        for q in range(4):
            start = heads[1 + q, d] * rows
            turned = pltpu.roll(code, (start - q * SUB + LANES) & (LANES - 1), 1)
            for m in range(tiles):
                at = (lanes + m * LANES) - start
                inside = at.astype(jnp.uint32) < rows
                inside = jnp.concatenate([inside] * bands, axis=0)
                sums[m] = jnp.where(inside, turned, sums[m])
        a = heads[0, d]
        for m in range(tiles):
            acc[a, :, m * LANES : (m + 1) * LANES] += sums[m] * scale
        return jnp.maximum(most, code[0:8])

    most = lax.fori_loop(0, devices, add, jnp.full((8, LANES), -8.0 * 1024, F32), unroll=32)
    most = jnp.broadcast_to(most[0:1, SUB + rows : SUB + rows + 1], (8, LANES))
    unit[...] = most
    inverse = jnp.exp2(FLOOR - most * 0.125)[0:1]
    rate = codes(devices)

    def send(a, carry):
        parts = []
        for m in range(tiles):
            value = acc[a, :, m * LANES : (m + 1) * LANES]
            size = jnp.log2(1.0 + jnp.abs(value) * inverse)
            parts.append(jnp.round(size * jnp.where(value < 0.0, -rate, rate)))
        out[owner[0, a]] = jnp.concatenate(parts, axis=0).astype(I16)
        return carry

    lax.fori_loop(0, aggs, send, 0, unroll=8)


def decode_kernel(unit, code, out, ready, sems):
    devices, rows, width = ready.shape
    parts = sems.shape[0]
    block = devices // parts
    delta = jnp.exp2(unit[0:1] * 0.125 - FLOOR)
    rate = 1.0 / codes(devices)

    def copy(g):
        here = pl.ds(g * block, block)
        return pltpu.make_async_copy(ready.at[here], out.at[here], sems.at[g])

    def step(g, carry):
        for j in range(block):
            d = g * block + j
            for m in range(width // LANES):
                x = code[d, rows * m : rows * (m + 1)].astype(F32)
                size = (jnp.exp2(jnp.abs(x) * rate) - 1.0) * jnp.where(x < 0.0, -delta, delta)
                ready[d, :, m * LANES : (m + 1) * LANES] = size
        copy(g).start()
        return carry

    lax.fori_loop(0, parts, step, 0)

    def finish(g, carry):
        copy(g).wait()
        return carry

    lax.fori_loop(0, parts, finish, 0)


def swap(x):
    return lax.all_to_all(x, AXES, split_axis=0, concat_axis=0, tiled=True)


def in_hbm(x):
    return pltpu.with_memory_space_constraint(x, pltpu.HBM)


def grant(mib):
    return pltpu.CompilerParams(vmem_limit_bytes=mib << 20)


def per_device(prolong, stiffness, request, col_slot, col_pos, coarse_owner):
    devices = lax.axis_size(AXES)
    aggs, rows, dof = prolong.shape
    per_row = stiffness.shape[1]
    width = MAXNB * rows
    smem = pl.BlockSpec(memory_space=pltpu.SMEM)
    vmem = pl.BlockSpec(memory_space=pltpu.VMEM)
    hbm = pl.BlockSpec(memory_space=pltpu.HBM)

    asking = jnp.concatenate([request[:, None], col_pos, col_pos[:, 0:3]], axis=1)
    asked = swap(asking[:, None, :])[:, 0, :]

    block = devices // 8
    picked, heads, near = pl.pallas_call(
        pick_kernel,
        out_shape=(
            jax.ShapeDtypeStruct((devices, rows, dof), BF16),
            jax.ShapeDtypeStruct((8, devices), I32),
            jax.ShapeDtypeStruct((block, per_row, dof, dof), BF16),
        ),
        in_specs=[vmem, hbm, hbm],
        out_specs=(vmem, vmem, vmem),
        scratch_shapes=[
            pltpu.VMEM((aggs, rows, dof), BF16),
            pltpu.SMEM((8, devices), I32),
            pltpu.SemaphoreType.DMA((6,)),
        ],
        compiler_params=grant(8),
        name="pick",
    )(asked, in_hbm(prolong), in_hbm(stiffness))
    fetched = swap(picked)

    sent = pl.pallas_call(
        partial_kernel,
        out_shape=jax.ShapeDtypeStruct((devices, rows, LANES), I16),
        in_specs=[smem, vmem, vmem, hbm],
        out_specs=vmem,
        scratch_shapes=[
            pltpu.VMEM((devices, SUB, dof), BF16),
            pltpu.VMEM((devices // 2, 2 * SUB, 2 * dof), BF16),
            pltpu.VMEM((devices - block, per_row, dof, dof), BF16),
            pltpu.SemaphoreType.DMA((devices // block - 1,)),
        ],
        compiler_params=grant(40),
        name="partial",
    )(in_hbm(col_slot.T), fetched, near, in_hbm(stiffness))
    blocks = swap(sent)

    depth = rows * (width // LANES)
    coarse, unit = pl.pallas_call(
        place_kernel,
        out_shape=(
            jax.ShapeDtypeStruct((devices, depth, LANES), I16),
            jax.ShapeDtypeStruct((8, LANES), F32),
        ),
        in_specs=[smem, smem, vmem],
        out_specs=(vmem, vmem),
        scratch_shapes=[pltpu.VMEM((aggs, rows, width), F32)],
        compiler_params=grant(16),
        name="place",
    )(heads, in_hbm(coarse_owner.T), blocks)
    arrived = swap(coarse)

    return pl.pallas_call(
        decode_kernel,
        out_shape=jax.ShapeDtypeStruct((devices, rows, width), F32),
        in_specs=[vmem, vmem],
        out_specs=hbm,
        scratch_shapes=[pltpu.VMEM((devices, rows, width), F32), pltpu.SemaphoreType.DMA((4,))],
        compiler_params=grant(16),
        name="decode",
    )(unit, arrived)


def solution(mesh):
    placed = (
        P(AXES, None, None),
        P(AXES, None, None, None),
        P(AXES),
        P(AXES, None),
        P(AXES, None),
        P(AXES, None),
    )
    return jax.shard_map(
        per_device, mesh=mesh, in_specs=placed, out_specs=P(AXES, None, None), check_vma=False
    )
```

```python
import math

import jax
import jax.numpy as jnp
from jax import lax
from jax.experimental import pallas as pl
from jax.experimental.pallas import tpu as pltpu
from jax.sharding import PartitionSpec as P

MAXNB = 16
AXES = ("gx", "gy")
F32 = jnp.float32
BF16 = jnp.bfloat16
I16 = jnp.int16
I32 = jnp.int32

TOP = 32766.0
TINY = 2.0**-100
FLOOR = 14
DEPTH = 4
LANES = 128
SUB = 32


def lane_ids(rows):
    return lax.broadcasted_iota(I32, (rows, LANES), 1)


def codes(devices):
    return TOP / (FLOOR + math.log2(devices))


def level(top):
    return jnp.ceil(8.0 * jnp.log2(jnp.maximum(top, TINY)))


def pick_kernel(asked, prolong, stiff, slot, owner, out, heads, held, named, sems):
    load = pltpu.make_async_copy(prolong, held, sems.at[0])
    load.start()
    heads[...] = asked[...].T
    name = pltpu.make_async_copy(heads, named, sems.at[1])
    name.start()
    name.wait()
    load.wait()

    def step(d, carry):
        out[d] = held[named[0, d]]
        return carry

    lax.fori_loop(0, out.shape[0], step, 0, unroll=16)


def partial_kernel(slot, fetched, stiff, out, padded, pairs):
    devices, rows, dof = fetched.shape
    per_row = stiff.shape[1]
    lanes = lane_ids(rows)
    def fill(p, carry):
        pairs[p] = jnp.zeros(pairs.shape[1:], BF16)
        for h in range(2):
            mine = fetched[2 * p + h]
            padded[2 * p + h, 0:rows, :] = mine
            padded[2 * p + h, rows:SUB, :] = jnp.zeros((SUB - rows, LANES), BF16)
            pairs[p, SUB * h : SUB * h + rows, LANES * h : LANES * (h + 1)] = mine
        return carry

    lax.fori_loop(0, devices // 2, fill, 0, unroll=4)

    def products(*accs):
        most = jnp.zeros((rows, 1), F32)

        def first(p):
            for c in range(2):
                tile = jnp.concatenate(
                    [
                        jnp.concatenate([stiff[2 * p + h, 2 * c], stiff[2 * p + h, 2 * c + 1]], axis=1)
                        for h in range(2)
                    ],
                    axis=0,
                )
                pltpu.matmul_push_rhs(tile, staging_register=c, mxu_index=0)
                pltpu.matmul_acc_lhs(accs[2 * (p % DEPTH) + c], pairs[p], load_staged_rhs=c)

        def second(p):
            both = [pltpu.matmul_pop(accs[2 * (p % DEPTH) + c]) for c in range(2)]
            lefts = []
            rights = []
            for h in range(2):
                highs = []
                lows = []
                for q in range(per_row):
                    w = both[q // 2][SUB * h : SUB * h + rows, (q % 2) * LANES : (q % 2 + 1) * LANES]
                    high = w.astype(BF16).astype(F32)
                    highs.append(high)
                    lows.append(w - high)
                lefts.append(
                    jnp.concatenate(
                        [jnp.concatenate(highs, axis=0).astype(BF16), jnp.concatenate(lows, axis=0).astype(BF16)],
                        axis=1,
                    )
                )
                rights += [padded[slot[q, 2 * p + h]] for q in range(per_row)]
            right = jnp.concatenate(rights, axis=0)
            right = jnp.concatenate([right, right], axis=1)
            pltpu.matmul_push_rhs(right, staging_register=p % 2, mxu_index=1, transpose=True)
            pltpu.matmul_acc_lhs(accs[2 * DEPTH + p % DEPTH], jnp.concatenate(lefts, axis=0), load_staged_rhs=p % 2)

        def third(p, most):
            prod = pltpu.matmul_pop(accs[2 * DEPTH + p % DEPTH])
            for h in range(2):
                mine = prod[h * per_row * rows : (h + 1) * per_row * rows, h * LANES : (h + 1) * LANES]
                value = mine[0:rows]
                for q in range(1, per_row):
                    value = jnp.where(lanes < q * SUB, value, mine[q * rows : (q + 1) * rows])
                top = jnp.max(jnp.abs(value), axis=1, keepdims=True)
                most = jnp.maximum(most, top)
                e = level(top)
                code = jnp.round(value * (jnp.exp2(e * -0.125) * TOP))
                code = jnp.where(lanes == rows, e, code)
                out[2 * p + h] = code.astype(I16)
            return most

        count = devices // 2
        for i in range(count + 2 * (DEPTH - 1)):
            if i < count:
                first(i)
            if 0 <= i - (DEPTH - 1) < count:
                second(i - (DEPTH - 1))
            if 0 <= i - 2 * (DEPTH - 1) < count:
                most = third(i - 2 * (DEPTH - 1), most)

        most = jnp.broadcast_to(level(jnp.max(most, axis=0, keepdims=True)), (8, LANES)).astype(I16)
        spare = lane_ids(8).astype(I16) == SUB + rows

        def share(t, carry):
            out[t, 0:8, :] = jnp.where(spare, most, out[t, 0:8, :])
            return carry

        lax.fori_loop(0, devices, share, 0, unroll=16)

    wide = 2 * LANES
    pl.run_scoped(
        products,
        *[pltpu.ACC(0)((2 * SUB, wide), F32) for _ in range(2 * DEPTH)],
        *[pltpu.ACC(1)((2 * per_row * rows, wide), F32) for _ in range(DEPTH)],
    )


def place_kernel(heads, owner, blocks, out, unit, acc):
    devices, rows, _ = blocks.shape
    aggs = acc.shape[0]
    tiles = acc.shape[2] // LANES
    lanes = lane_ids(8)
    bands = rows // 8

    def clear(a, carry):
        acc[a] = jnp.zeros(acc.shape[1:], F32)
        return carry

    lax.fori_loop(0, aggs, clear, 0, unroll=8)

    def clear_out(d, carry):
        out[d] = jnp.zeros(out.shape[1:], I16)
        return carry

    lax.fori_loop(0, devices, clear_out, 0, unroll=8)

    def add(d, most):
        code = blocks[d].astype(F32)
        scale = jnp.exp2(code[:, rows : rows + 1] * 0.125) * (1.0 / TOP)
        sums = [jnp.zeros((rows, LANES), F32) for _ in range(tiles)]
        for q in range(4):
            start = heads[1 + q, d] * rows
            turned = pltpu.roll(code, (start - q * SUB + LANES) & (LANES - 1), 1)
            for m in range(tiles):
                at = (lanes + m * LANES) - start
                inside = at.astype(jnp.uint32) < rows
                inside = jnp.concatenate([inside] * bands, axis=0)
                sums[m] = jnp.where(inside, turned, sums[m])
        a = heads[0, d]
        for m in range(tiles):
            acc[a, :, m * LANES : (m + 1) * LANES] += sums[m] * scale
        return jnp.maximum(most, code[0:8])

    most = lax.fori_loop(0, devices, add, jnp.full((8, LANES), -8.0 * 1024, F32), unroll=32)
    most = jnp.broadcast_to(most[0:1, SUB + rows : SUB + rows + 1], (8, LANES))
    unit[...] = most
    inverse = jnp.exp2(FLOOR - most * 0.125)[0:1]
    rate = codes(devices)

    def send(a, carry):
        parts = []
        for m in range(tiles):
            value = acc[a, :, m * LANES : (m + 1) * LANES]
            size = jnp.log2(1.0 + jnp.abs(value) * inverse)
            parts.append(jnp.round(size * jnp.where(value < 0.0, -rate, rate)))
        out[owner[0, a]] = jnp.concatenate(parts, axis=0).astype(I16)
        return carry

    lax.fori_loop(0, aggs, send, 0, unroll=8)


def decode_kernel(unit, code, out, ready, sems):
    devices, rows, width = ready.shape
    parts = sems.shape[0]
    block = devices // parts
    delta = jnp.exp2(unit[0:1] * 0.125 - FLOOR)
    rate = 1.0 / codes(devices)

    def copy(g):
        here = pl.ds(g * block, block)
        return pltpu.make_async_copy(ready.at[here], out.at[here], sems.at[g])

    def step(g, carry):
        for j in range(block):
            d = g * block + j
            for m in range(width // LANES):
                x = code[d, rows * m : rows * (m + 1)].astype(F32)
                size = (jnp.exp2(jnp.abs(x) * rate) - 1.0) * jnp.where(x < 0.0, -delta, delta)
                ready[d, :, m * LANES : (m + 1) * LANES] = size
        copy(g).start()
        return carry

    lax.fori_loop(0, parts, step, 0)

    def finish(g, carry):
        copy(g).wait()
        return carry

    lax.fori_loop(0, parts, finish, 0)


def swap(x):
    return lax.all_to_all(x, AXES, split_axis=0, concat_axis=0, tiled=True)


def in_hbm(x):
    return pltpu.with_memory_space_constraint(x, pltpu.HBM)


def on_chip(x):
    return pltpu.with_memory_space_constraint(x, pltpu.VMEM)


def grant(mib):
    return pltpu.CompilerParams(vmem_limit_bytes=mib << 20)


def per_device(prolong, stiffness, request, col_slot, col_pos, coarse_owner):
    devices = lax.axis_size(AXES)
    aggs, rows, dof = prolong.shape
    per_row = stiffness.shape[1]
    width = MAXNB * rows
    smem = pl.BlockSpec(memory_space=pltpu.SMEM)
    vmem = pl.BlockSpec(memory_space=pltpu.VMEM)
    hbm = pl.BlockSpec(memory_space=pltpu.HBM)

    asking = jnp.concatenate([request[:, None], col_pos, col_pos[:, 0:3]], axis=1)
    asked = swap(asking[:, None, :])[:, 0, :]

    picked, heads = pl.pallas_call(
        pick_kernel,
        out_shape=(
            jax.ShapeDtypeStruct((devices, rows, dof), BF16),
            jax.ShapeDtypeStruct((8, devices), I32),
        ),
        in_specs=[vmem, hbm, hbm, hbm, hbm],
        out_specs=(vmem, vmem),
        scratch_shapes=[
            pltpu.VMEM((aggs, rows, dof), BF16),
            pltpu.SMEM((8, devices), I32),
            pltpu.SemaphoreType.DMA((2,)),
        ],
        compiler_params=grant(4),
        name="pick",
    )(asked, in_hbm(prolong), in_hbm(stiffness), in_hbm(col_slot.T), in_hbm(coarse_owner.T))
    fetched = swap(picked)

    sent = pl.pallas_call(
        partial_kernel,
        out_shape=jax.ShapeDtypeStruct((devices, rows, LANES), I16),
        in_specs=[smem, vmem, vmem],
        out_specs=vmem,
        scratch_shapes=[
            pltpu.VMEM((devices, SUB, dof), BF16),
            pltpu.VMEM((devices // 2, 2 * SUB, 2 * dof), BF16),
        ],
        compiler_params=grant(16),
        name="partial",
    )(on_chip(col_slot.T), fetched, on_chip(stiffness))
    blocks = swap(sent)

    depth = rows * (width // LANES)
    coarse, unit = pl.pallas_call(
        place_kernel,
        out_shape=(
            jax.ShapeDtypeStruct((devices, depth, LANES), I16),
            jax.ShapeDtypeStruct((8, LANES), F32),
        ),
        in_specs=[smem, smem, vmem],
        out_specs=(vmem, vmem),
        scratch_shapes=[pltpu.VMEM((aggs, rows, width), F32)],
        compiler_params=grant(16),
        name="place",
    )(heads, on_chip(coarse_owner.T), blocks)
    arrived = swap(coarse)

    return pl.pallas_call(
        decode_kernel,
        out_shape=jax.ShapeDtypeStruct((devices, rows, width), F32),
        in_specs=[vmem, vmem],
        out_specs=hbm,
        scratch_shapes=[pltpu.VMEM((devices, rows, width), F32), pltpu.SemaphoreType.DMA((4,))],
        compiler_params=grant(16),
        name="decode",
    )(unit, arrived)


def solution(mesh):
    placed = (
        P(AXES, None, None),
        P(AXES, None, None, None),
        P(AXES),
        P(AXES, None),
        P(AXES, None),
        P(AXES, None),
    )
    return jax.shard_map(
        per_device, mesh=mesh, in_specs=placed, out_specs=P(AXES, None, None), check_vma=False
    )
```

```python
import math

import jax
import jax.numpy as jnp
from jax import lax
from jax.experimental import pallas as pl
from jax.experimental.pallas import tpu as pltpu
from jax.sharding import PartitionSpec as P

MAXNB = 16
AXES = ("gx", "gy")
F32 = jnp.float32
BF16 = jnp.bfloat16
I16 = jnp.int16
I32 = jnp.int32

TOP = 32766.0
TINY = 2.0**-100
FLOOR = 14
DEPTH = 4
LANES = 128
SUB = 32


def lane_ids(rows):
    return lax.broadcasted_iota(I32, (rows, LANES), 1)


def codes(devices):
    return TOP / (FLOOR + math.log2(devices))


def level(top):
    return jnp.ceil(8.0 * jnp.log2(jnp.maximum(top, TINY)))


def pick_kernel(asked, prolong, stiff, slot, owner, out, heads, blank, clean, held, named, sems):
    load = pltpu.make_async_copy(prolong, held, sems.at[0])
    load.start()
    heads[...] = asked[...].T
    name = pltpu.make_async_copy(heads, named, sems.at[1])
    name.start()

    def clear_sums(a, carry):
        clean[a] = jnp.zeros(clean.shape[1:], F32)
        return carry

    lax.fori_loop(0, clean.shape[0], clear_sums, 0, unroll=8)

    def clear_rows(d, carry):
        blank[d] = jnp.zeros(blank.shape[1:], I16)
        return carry

    lax.fori_loop(0, blank.shape[0], clear_rows, 0, unroll=8)
    name.wait()
    load.wait()

    def step(d, carry):
        out[d] = held[named[0, d]]
        return carry

    lax.fori_loop(0, out.shape[0], step, 0, unroll=16)


def partial_kernel(slot, fetched, stiff, out, padded, pairs):
    devices, rows, dof = fetched.shape
    per_row = stiff.shape[1]
    lanes = lane_ids(rows)
    def fill(p, carry):
        pairs[p] = jnp.zeros(pairs.shape[1:], BF16)
        for h in range(2):
            mine = fetched[2 * p + h]
            padded[2 * p + h, 0:rows, :] = mine
            padded[2 * p + h, rows:SUB, :] = jnp.zeros((SUB - rows, LANES), BF16)
            pairs[p, SUB * h : SUB * h + rows, LANES * h : LANES * (h + 1)] = mine
        return carry

    lax.fori_loop(0, devices // 2, fill, 0, unroll=4)

    def products(*accs):
        most = jnp.zeros((rows, 1), F32)

        def first(p):
            for c in range(2):
                tile = jnp.concatenate(
                    [
                        jnp.concatenate([stiff[2 * p + h, 2 * c], stiff[2 * p + h, 2 * c + 1]], axis=1)
                        for h in range(2)
                    ],
                    axis=0,
                )
                pltpu.matmul_push_rhs(tile, staging_register=c, mxu_index=0)
                pltpu.matmul_acc_lhs(accs[2 * (p % DEPTH) + c], pairs[p], load_staged_rhs=c)

        def second(p):
            both = [pltpu.matmul_pop(accs[2 * (p % DEPTH) + c]) for c in range(2)]
            lefts = []
            rights = []
            for h in range(2):
                highs = []
                lows = []
                for q in range(per_row):
                    w = both[q // 2][SUB * h : SUB * h + rows, (q % 2) * LANES : (q % 2 + 1) * LANES]
                    high = w.astype(BF16).astype(F32)
                    highs.append(high)
                    lows.append(w - high)
                lefts.append(
                    jnp.concatenate(
                        [jnp.concatenate(highs, axis=0).astype(BF16), jnp.concatenate(lows, axis=0).astype(BF16)],
                        axis=1,
                    )
                )
                rights += [padded[slot[q, 2 * p + h]] for q in range(per_row)]
            right = jnp.concatenate(rights, axis=0)
            right = jnp.concatenate([right, right], axis=1)
            pltpu.matmul_push_rhs(right, staging_register=p % 2, mxu_index=1, transpose=True)
            pltpu.matmul_acc_lhs(accs[2 * DEPTH + p % DEPTH], jnp.concatenate(lefts, axis=0), load_staged_rhs=p % 2)

        def third(p, most):
            prod = pltpu.matmul_pop(accs[2 * DEPTH + p % DEPTH])
            for h in range(2):
                mine = prod[h * per_row * rows : (h + 1) * per_row * rows, h * LANES : (h + 1) * LANES]
                value = mine[0:rows]
                for q in range(1, per_row):
                    value = jnp.where(lanes < q * SUB, value, mine[q * rows : (q + 1) * rows])
                top = jnp.max(jnp.abs(value), axis=1, keepdims=True)
                most = jnp.maximum(most, top)
                e = level(top)
                code = jnp.round(value * (jnp.exp2(e * -0.125) * TOP))
                code = jnp.where(lanes == rows, e, code)
                out[2 * p + h] = code.astype(I16)
            return most

        count = devices // 2
        for i in range(count + 2 * (DEPTH - 1)):
            if i < count:
                first(i)
            if 0 <= i - (DEPTH - 1) < count:
                second(i - (DEPTH - 1))
            if 0 <= i - 2 * (DEPTH - 1) < count:
                most = third(i - 2 * (DEPTH - 1), most)

        most = jnp.broadcast_to(level(jnp.max(most, axis=0, keepdims=True)), (8, LANES)).astype(I16)
        spare = lane_ids(8).astype(I16) == SUB + rows

        def share(t, carry):
            out[t, 0:8, :] = jnp.where(spare, most, out[t, 0:8, :])
            return carry

        lax.fori_loop(0, devices, share, 0, unroll=16)

    wide = 2 * LANES
    pl.run_scoped(
        products,
        *[pltpu.ACC(0)((2 * SUB, wide), F32) for _ in range(2 * DEPTH)],
        *[pltpu.ACC(1)((2 * per_row * rows, wide), F32) for _ in range(DEPTH)],
    )


def place_kernel(heads, owner, blocks, blank, clean, out, unit, acc):
    devices, rows, _ = blocks.shape
    aggs = acc.shape[0]
    tiles = acc.shape[2] // LANES
    lanes = lane_ids(8)
    bands = rows // 8

    def add(d, most):
        code = blocks[d].astype(F32)
        scale = jnp.exp2(code[:, rows : rows + 1] * 0.125) * (1.0 / TOP)
        sums = [jnp.zeros((rows, LANES), F32) for _ in range(tiles)]
        for q in range(4):
            start = heads[1 + q, d] * rows
            turned = pltpu.roll(code, (start - q * SUB + LANES) & (LANES - 1), 1)
            for m in range(tiles):
                at = (lanes + m * LANES) - start
                inside = at.astype(jnp.uint32) < rows
                inside = jnp.concatenate([inside] * bands, axis=0)
                sums[m] = jnp.where(inside, turned, sums[m])
        a = heads[0, d]
        for m in range(tiles):
            acc[a, :, m * LANES : (m + 1) * LANES] += sums[m] * scale
        return jnp.maximum(most, code[0:8])

    most = lax.fori_loop(0, devices, add, jnp.full((8, LANES), -8.0 * 1024, F32), unroll=128)
    most = jnp.broadcast_to(most[0:1, SUB + rows : SUB + rows + 1], (8, LANES))
    unit[...] = most
    inverse = jnp.exp2(FLOOR - most * 0.125)[0:1]
    rate = codes(devices)

    def send(a, carry):
        parts = []
        for m in range(tiles):
            value = acc[a, :, m * LANES : (m + 1) * LANES]
            size = jnp.log2(1.0 + jnp.abs(value) * inverse)
            parts.append(jnp.round(size * jnp.where(value < 0.0, -rate, rate)))
        out[owner[0, a]] = jnp.concatenate(parts, axis=0).astype(I16)
        return carry

    lax.fori_loop(0, aggs, send, 0, unroll=64)


def decode_kernel(unit, code, out, ready, sems):
    devices, rows, width = ready.shape
    parts = sems.shape[0]
    block = devices // parts
    delta = jnp.exp2(unit[0:1] * 0.125 - FLOOR)
    rate = 1.0 / codes(devices)

    def copy(g):
        here = pl.ds(g * block, block)
        return pltpu.make_async_copy(ready.at[here], out.at[here], sems.at[g])

    def step(g, carry):
        for j in range(block):
            d = g * block + j
            for m in range(width // LANES):
                x = code[d, rows * m : rows * (m + 1)].astype(F32)
                size = (jnp.exp2(jnp.abs(x) * rate) - 1.0) * jnp.where(x < 0.0, -delta, delta)
                ready[d, :, m * LANES : (m + 1) * LANES] = size
        copy(g).start()
        return carry

    lax.fori_loop(0, parts, step, 0)

    def finish(g, carry):
        copy(g).wait()
        return carry

    lax.fori_loop(0, parts, finish, 0)


def swap(x):
    return lax.all_to_all(x, AXES, split_axis=0, concat_axis=0, tiled=True)


def in_hbm(x):
    return pltpu.with_memory_space_constraint(x, pltpu.HBM)


def on_chip(x):
    return pltpu.with_memory_space_constraint(x, pltpu.VMEM)


def grant(mib):
    return pltpu.CompilerParams(vmem_limit_bytes=mib << 20)


def per_device(prolong, stiffness, request, col_slot, col_pos, coarse_owner):
    devices = lax.axis_size(AXES)
    aggs, rows, dof = prolong.shape
    per_row = stiffness.shape[1]
    width = MAXNB * rows
    smem = pl.BlockSpec(memory_space=pltpu.SMEM)
    vmem = pl.BlockSpec(memory_space=pltpu.VMEM)
    hbm = pl.BlockSpec(memory_space=pltpu.HBM)

    asking = jnp.concatenate([request[:, None], col_pos, col_pos[:, 0:3]], axis=1)
    asked = swap(asking[:, None, :])[:, 0, :]

    depth = rows * (width // LANES)
    picked, heads, blank, clean = pl.pallas_call(
        pick_kernel,
        out_shape=(
            jax.ShapeDtypeStruct((devices, rows, dof), BF16),
            jax.ShapeDtypeStruct((8, devices), I32),
            jax.ShapeDtypeStruct((devices, depth, LANES), I16),
            jax.ShapeDtypeStruct((aggs, rows, width), F32),
        ),
        in_specs=[vmem, hbm, hbm, hbm, hbm],
        out_specs=(vmem, vmem, vmem, vmem),
        scratch_shapes=[
            pltpu.VMEM((aggs, rows, dof), BF16),
            pltpu.SMEM((8, devices), I32),
            pltpu.SemaphoreType.DMA((2,)),
        ],
        compiler_params=grant(8),
        name="pick",
    )(asked, in_hbm(prolong), in_hbm(stiffness), in_hbm(col_slot.T), in_hbm(coarse_owner.T))
    fetched = swap(picked)

    sent = pl.pallas_call(
        partial_kernel,
        out_shape=jax.ShapeDtypeStruct((devices, rows, LANES), I16),
        in_specs=[smem, vmem, vmem],
        out_specs=vmem,
        scratch_shapes=[
            pltpu.VMEM((devices, SUB, dof), BF16),
            pltpu.VMEM((devices // 2, 2 * SUB, 2 * dof), BF16),
        ],
        compiler_params=grant(16),
        name="partial",
    )(on_chip(col_slot.T), fetched, on_chip(stiffness))
    blocks = swap(sent)

    coarse, unit, _ = pl.pallas_call(
        place_kernel,
        out_shape=(
            jax.ShapeDtypeStruct((devices, depth, LANES), I16),
            jax.ShapeDtypeStruct((8, LANES), F32),
            jax.ShapeDtypeStruct((aggs, rows, width), F32),
        ),
        in_specs=[smem, smem, vmem, vmem, vmem],
        out_specs=(vmem, vmem, vmem),
        input_output_aliases={3: 0, 4: 2},
        compiler_params=grant(8),
        name="place",
    )(heads, on_chip(coarse_owner.T), blocks, blank, clean)
    arrived = swap(coarse)

    return pl.pallas_call(
        decode_kernel,
        out_shape=jax.ShapeDtypeStruct((devices, rows, width), F32),
        in_specs=[vmem, vmem],
        out_specs=hbm,
        scratch_shapes=[pltpu.VMEM((devices, rows, width), F32), pltpu.SemaphoreType.DMA((4,))],
        compiler_params=grant(16),
        name="decode",
    )(unit, arrived)


def solution(mesh):
    placed = (
        P(AXES, None, None),
        P(AXES, None, None, None),
        P(AXES),
        P(AXES, None),
        P(AXES, None),
        P(AXES, None),
    )
    return jax.shard_map(
        per_device, mesh=mesh, in_specs=placed, out_specs=P(AXES, None, None), check_vma=False
    )
```

```python
import math

import jax
import jax.numpy as jnp
from jax import lax
from jax.experimental import pallas as pl
from jax.experimental.pallas import tpu as pltpu
from jax.sharding import PartitionSpec as P

MAXNB = 16
AXES = ("gx", "gy")
F32 = jnp.float32
BF16 = jnp.bfloat16
I16 = jnp.int16
I32 = jnp.int32

TOP = 32766.0
TINY = 2.0**-100
FLOOR = 14
DEPTH = 4
LANES = 128
SUB = 32


def lane_ids(rows):
    return lax.broadcasted_iota(I32, (rows, LANES), 1)


def codes(devices):
    return TOP / (FLOOR + math.log2(devices))


def level(top):
    return jnp.ceil(8.0 * jnp.log2(jnp.maximum(top, TINY)))


def pick_kernel(asked, prolong, stiff, slot, owner, out, heads, blank, clean, held, named, sems):
    load = pltpu.make_async_copy(prolong, held, sems.at[0])
    load.start()
    heads[...] = asked[...].T
    name = pltpu.make_async_copy(heads, named, sems.at[1])
    name.start()

    def clear_sums(a, carry):
        clean[a] = jnp.zeros(clean.shape[1:], F32)
        return carry

    lax.fori_loop(0, clean.shape[0], clear_sums, 0, unroll=8)

    def clear_rows(d, carry):
        blank[d] = jnp.zeros(blank.shape[1:], I16)
        return carry

    lax.fori_loop(0, blank.shape[0], clear_rows, 0, unroll=8)
    name.wait()
    load.wait()

    def step(d, carry):
        out[d] = held[named[0, d]]
        return carry

    lax.fori_loop(0, out.shape[0], step, 0, unroll=16)


def partial_kernel(slot, fetched, stiff, out, padded):
    devices, rows, dof = fetched.shape
    per_row = stiff.shape[1]
    lanes = lane_ids(rows)
    def fill(t, carry):
        padded[t, 0:rows, :] = fetched[t]
        padded[t, rows:SUB, :] = jnp.zeros((SUB - rows, LANES), BF16)
        return carry

    lax.fori_loop(0, devices, fill, 0, unroll=16)
    none = jnp.zeros((SUB, LANES), BF16)

    def products(*accs):
        most = jnp.zeros((rows, 1), F32)

        def first(p):
            left = jnp.concatenate(
                [
                    jnp.concatenate([padded[2 * p], none], axis=1),
                    jnp.concatenate([none, padded[2 * p + 1]], axis=1),
                ],
                axis=0,
            )
            for c in range(2):
                tile = jnp.concatenate(
                    [
                        jnp.concatenate([stiff[2 * p + h, 2 * c], stiff[2 * p + h, 2 * c + 1]], axis=1)
                        for h in range(2)
                    ],
                    axis=0,
                )
                pltpu.matmul_push_rhs(tile, staging_register=c, mxu_index=0)
                pltpu.matmul_acc_lhs(accs[2 * (p % DEPTH) + c], left, load_staged_rhs=c)

        def second(p):
            both = [pltpu.matmul_pop(accs[2 * (p % DEPTH) + c]) for c in range(2)]
            lefts = []
            rights = []
            for h in range(2):
                highs = []
                lows = []
                for q in range(per_row):
                    w = both[q // 2][SUB * h : SUB * h + rows, (q % 2) * LANES : (q % 2 + 1) * LANES]
                    high = w.astype(BF16).astype(F32)
                    highs.append(high)
                    lows.append(w - high)
                lefts.append(
                    jnp.concatenate(
                        [jnp.concatenate(highs, axis=0).astype(BF16), jnp.concatenate(lows, axis=0).astype(BF16)],
                        axis=1,
                    )
                )
                rights += [padded[slot[q, 2 * p + h]] for q in range(per_row)]
            right = jnp.concatenate(rights, axis=0)
            right = jnp.concatenate([right, right], axis=1)
            pltpu.matmul_push_rhs(right, staging_register=p % 2, mxu_index=1, transpose=True)
            pltpu.matmul_acc_lhs(accs[2 * DEPTH + p % DEPTH], jnp.concatenate(lefts, axis=0), load_staged_rhs=p % 2)

        def third(p, most):
            prod = pltpu.matmul_pop(accs[2 * DEPTH + p % DEPTH])
            for h in range(2):
                mine = prod[h * per_row * rows : (h + 1) * per_row * rows, h * LANES : (h + 1) * LANES]
                value = mine[0:rows]
                for q in range(1, per_row):
                    value = jnp.where(lanes < q * SUB, value, mine[q * rows : (q + 1) * rows])
                top = jnp.max(jnp.abs(value), axis=1, keepdims=True)
                most = jnp.maximum(most, top)
                e = level(top)
                code = jnp.round(value * (jnp.exp2(e * -0.125) * TOP))
                code = jnp.where(lanes == rows, e, code)
                out[2 * p + h] = code.astype(I16)
            return most

        count = devices // 2
        for i in range(count + 2 * (DEPTH - 1)):
            if i < count:
                first(i)
            if 0 <= i - (DEPTH - 1) < count:
                second(i - (DEPTH - 1))
            if 0 <= i - 2 * (DEPTH - 1) < count:
                most = third(i - 2 * (DEPTH - 1), most)

        most = jnp.broadcast_to(level(jnp.max(most, axis=0, keepdims=True)), (8, LANES)).astype(I16)
        spare = lane_ids(8).astype(I16) == SUB + rows

        def share(t, carry):
            out[t, 0:8, :] = jnp.where(spare, most, out[t, 0:8, :])
            return carry

        lax.fori_loop(0, devices, share, 0, unroll=16)

    wide = 2 * LANES
    pl.run_scoped(
        products,
        *[pltpu.ACC(0)((2 * SUB, wide), F32) for _ in range(2 * DEPTH)],
        *[pltpu.ACC(1)((2 * per_row * rows, wide), F32) for _ in range(DEPTH)],
    )


def place_kernel(heads, owner, blocks, blank, clean, out, unit, acc):
    devices, rows, _ = blocks.shape
    aggs = acc.shape[0]
    tiles = acc.shape[2] // LANES
    lanes = lane_ids(8)
    bands = rows // 8

    def add(d, most):
        code = blocks[d].astype(F32)
        scale = jnp.exp2(code[:, rows : rows + 1] * 0.125) * (1.0 / TOP)
        sums = [jnp.zeros((rows, LANES), F32) for _ in range(tiles)]
        for q in range(4):
            start = heads[1 + q, d] * rows
            turned = pltpu.roll(code, (start - q * SUB + LANES) & (LANES - 1), 1)
            for m in range(tiles):
                at = (lanes + m * LANES) - start
                inside = at.astype(jnp.uint32) < rows
                inside = jnp.concatenate([inside] * bands, axis=0)
                sums[m] = jnp.where(inside, turned, sums[m])
        a = heads[0, d]
        for m in range(tiles):
            acc[a, :, m * LANES : (m + 1) * LANES] += sums[m] * scale
        return jnp.maximum(most, code[0:8])

    most = lax.fori_loop(0, devices, add, jnp.full((8, LANES), -8.0 * 1024, F32), unroll=128)
    most = jnp.broadcast_to(most[0:1, SUB + rows : SUB + rows + 1], (8, LANES))
    unit[...] = most
    inverse = jnp.exp2(FLOOR - most * 0.125)[0:1]
    rate = codes(devices)

    def send(a, carry):
        parts = []
        for m in range(tiles):
            value = acc[a, :, m * LANES : (m + 1) * LANES]
            size = jnp.log2(1.0 + jnp.abs(value) * inverse)
            parts.append(jnp.round(size * jnp.where(value < 0.0, -rate, rate)))
        out[owner[0, a]] = jnp.concatenate(parts, axis=0).astype(I16)
        return carry

    lax.fori_loop(0, aggs, send, 0, unroll=64)


def decode_kernel(unit, code, out, ready, sems):
    devices, rows, width = ready.shape
    parts = sems.shape[0]
    block = devices // parts
    delta = jnp.exp2(unit[0:1] * 0.125 - FLOOR)
    rate = 1.0 / codes(devices)

    def copy(g):
        here = pl.ds(g * block, block)
        return pltpu.make_async_copy(ready.at[here], out.at[here], sems.at[g])

    def step(g, carry):
        for j in range(block):
            d = g * block + j
            for m in range(width // LANES):
                x = code[d, rows * m : rows * (m + 1)].astype(F32)
                size = (jnp.exp2(jnp.abs(x) * rate) - 1.0) * jnp.where(x < 0.0, -delta, delta)
                ready[d, :, m * LANES : (m + 1) * LANES] = size
        copy(g).start()
        return carry

    lax.fori_loop(0, parts, step, 0)

    def finish(g, carry):
        copy(g).wait()
        return carry

    lax.fori_loop(0, parts, finish, 0)


def swap(x):
    return lax.all_to_all(x, AXES, split_axis=0, concat_axis=0, tiled=True)


def in_hbm(x):
    return pltpu.with_memory_space_constraint(x, pltpu.HBM)


def on_chip(x):
    return pltpu.with_memory_space_constraint(x, pltpu.VMEM)


def grant(mib):
    return pltpu.CompilerParams(vmem_limit_bytes=mib << 20)


def per_device(prolong, stiffness, request, col_slot, col_pos, coarse_owner):
    devices = lax.axis_size(AXES)
    aggs, rows, dof = prolong.shape
    per_row = stiffness.shape[1]
    width = MAXNB * rows
    smem = pl.BlockSpec(memory_space=pltpu.SMEM)
    vmem = pl.BlockSpec(memory_space=pltpu.VMEM)
    hbm = pl.BlockSpec(memory_space=pltpu.HBM)

    asking = jnp.concatenate([request[:, None], col_pos, col_pos[:, 0:3]], axis=1)
    asked = swap(asking[:, None, :])[:, 0, :]

    depth = rows * (width // LANES)
    picked, heads, blank, clean = pl.pallas_call(
        pick_kernel,
        out_shape=(
            jax.ShapeDtypeStruct((devices, rows, dof), BF16),
            jax.ShapeDtypeStruct((8, devices), I32),
            jax.ShapeDtypeStruct((devices, depth, LANES), I16),
            jax.ShapeDtypeStruct((aggs, rows, width), F32),
        ),
        in_specs=[vmem, hbm, hbm, hbm, hbm],
        out_specs=(vmem, vmem, vmem, vmem),
        scratch_shapes=[
            pltpu.VMEM((aggs, rows, dof), BF16),
            pltpu.SMEM((8, devices), I32),
            pltpu.SemaphoreType.DMA((2,)),
        ],
        compiler_params=grant(8),
        name="pick",
    )(asked, in_hbm(prolong), in_hbm(stiffness), in_hbm(col_slot.T), in_hbm(coarse_owner.T))
    fetched = swap(picked)

    sent = pl.pallas_call(
        partial_kernel,
        out_shape=jax.ShapeDtypeStruct((devices, rows, LANES), I16),
        in_specs=[smem, vmem, vmem],
        out_specs=vmem,
        scratch_shapes=[pltpu.VMEM((devices, SUB, dof), BF16)],
        compiler_params=grant(16),
        name="partial",
    )(on_chip(col_slot.T), fetched, on_chip(stiffness))
    blocks = swap(sent)

    coarse, unit, _ = pl.pallas_call(
        place_kernel,
        out_shape=(
            jax.ShapeDtypeStruct((devices, depth, LANES), I16),
            jax.ShapeDtypeStruct((8, LANES), F32),
            jax.ShapeDtypeStruct((aggs, rows, width), F32),
        ),
        in_specs=[smem, smem, vmem, vmem, vmem],
        out_specs=(vmem, vmem, vmem),
        input_output_aliases={3: 0, 4: 2},
        compiler_params=grant(8),
        name="place",
    )(heads, on_chip(coarse_owner.T), blocks, blank, clean)
    arrived = swap(coarse)

    return pl.pallas_call(
        decode_kernel,
        out_shape=jax.ShapeDtypeStruct((devices, rows, width), F32),
        in_specs=[vmem, vmem],
        out_specs=hbm,
        scratch_shapes=[pltpu.VMEM((devices, rows, width), F32), pltpu.SemaphoreType.DMA((4,))],
        compiler_params=grant(16),
        name="decode",
    )(unit, arrived)


def solution(mesh):
    placed = (
        P(AXES, None, None),
        P(AXES, None, None, None),
        P(AXES),
        P(AXES, None),
        P(AXES, None),
        P(AXES, None),
    )
    return jax.shard_map(
        per_device, mesh=mesh, in_specs=placed, out_specs=P(AXES, None, None), check_vma=False
    )
```

```python
import math

import jax
import jax.numpy as jnp
from jax import lax
from jax.experimental import pallas as pl
from jax.experimental.pallas import tpu as pltpu
from jax.sharding import PartitionSpec as P

MAXNB = 16
AXES = ("gx", "gy")
F32 = jnp.float32
BF16 = jnp.bfloat16
I16 = jnp.int16
I32 = jnp.int32

TOP = 32766.0
TINY = 2.0**-100
FLOOR = 14
DEPTH = 4
LANES = 128
SUB = 32


def lane_ids(rows):
    return lax.broadcasted_iota(I32, (rows, LANES), 1)


def codes(devices):
    return TOP / (FLOOR + math.log2(devices))


def level(top):
    return jnp.ceil(8.0 * jnp.log2(jnp.maximum(top, TINY)))


def pick_kernel(asked, prolong, stiff, slot, owner, out, heads, blank, clean, held, named, sems):
    load = pltpu.make_async_copy(prolong, held, sems.at[0])
    load.start()
    heads[0 : asked.shape[1], :] = asked[...].T
    heads[asked.shape[1] :, :] = jnp.zeros((8 - asked.shape[1], LANES), I32)
    name = pltpu.make_async_copy(heads, named, sems.at[1])
    name.start()

    def clear_sums(a, carry):
        clean[a] = jnp.zeros(clean.shape[1:], F32)
        return carry

    lax.fori_loop(0, clean.shape[0], clear_sums, 0, unroll=8)

    def clear_rows(d, carry):
        blank[d] = jnp.zeros(blank.shape[1:], I16)
        return carry

    lax.fori_loop(0, blank.shape[0], clear_rows, 0, unroll=8)
    name.wait()
    load.wait()

    def step(d, carry):
        out[d] = held[named[0, d]]
        return carry

    lax.fori_loop(0, out.shape[0], step, 0, unroll=16)


def partial_kernel(slot, fetched, stiff, out, padded):
    devices, rows, dof = fetched.shape
    per_row = stiff.shape[1]
    lanes = lane_ids(rows)
    def fill(t, carry):
        padded[t, 0:rows, :] = fetched[t]
        padded[t, rows:SUB, :] = jnp.zeros((SUB - rows, LANES), BF16)
        return carry

    lax.fori_loop(0, devices, fill, 0, unroll=32)
    none = jnp.zeros((SUB, LANES), BF16)

    def products(*accs):
        most = jnp.zeros((rows, 1), F32)

        def first(p):
            left = jnp.concatenate(
                [
                    jnp.concatenate([padded[2 * p], none], axis=1),
                    jnp.concatenate([none, padded[2 * p + 1]], axis=1),
                ],
                axis=0,
            )
            for c in range(2):
                tile = jnp.concatenate(
                    [
                        jnp.concatenate([stiff[2 * p + h, 2 * c], stiff[2 * p + h, 2 * c + 1]], axis=1)
                        for h in range(2)
                    ],
                    axis=0,
                )
                pltpu.matmul_push_rhs(tile, staging_register=c, mxu_index=0)
                pltpu.matmul_acc_lhs(accs[2 * (p % DEPTH) + c], left, load_staged_rhs=c)

        def second(p):
            both = [pltpu.matmul_pop(accs[2 * (p % DEPTH) + c]) for c in range(2)]
            lefts = []
            rights = []
            for h in range(2):
                highs = []
                lows = []
                for q in range(per_row):
                    w = both[q // 2][SUB * h : SUB * h + rows, (q % 2) * LANES : (q % 2 + 1) * LANES]
                    high = w.astype(BF16).astype(F32)
                    highs.append(high)
                    lows.append(w - high)
                lefts.append(
                    jnp.concatenate(
                        [jnp.concatenate(highs, axis=0).astype(BF16), jnp.concatenate(lows, axis=0).astype(BF16)],
                        axis=1,
                    )
                )
                rights += [padded[slot[q, 2 * p + h]] for q in range(per_row)]
            right = jnp.concatenate(rights, axis=0)
            right = jnp.concatenate([right, right], axis=1)
            pltpu.matmul_push_rhs(right, staging_register=p % 2, mxu_index=1, transpose=True)
            pltpu.matmul_acc_lhs(accs[2 * DEPTH + p % DEPTH], jnp.concatenate(lefts, axis=0), load_staged_rhs=p % 2)

        def third(p, most):
            prod = pltpu.matmul_pop(accs[2 * DEPTH + p % DEPTH])
            for h in range(2):
                mine = prod[h * per_row * rows : (h + 1) * per_row * rows, h * LANES : (h + 1) * LANES]
                value = mine[0:rows]
                for q in range(1, per_row):
                    value = jnp.where(lanes < q * SUB, value, mine[q * rows : (q + 1) * rows])
                top = jnp.max(jnp.abs(value), axis=1, keepdims=True)
                most = jnp.maximum(most, top)
                e = level(top)
                code = jnp.round(value * (jnp.exp2(e * -0.125) * TOP))
                code = jnp.where(lanes == rows, e, code)
                out[2 * p + h] = code.astype(I16)
            return most

        count = devices // 2
        for i in range(count + 2 * (DEPTH - 1)):
            if i < count:
                first(i)
            if 0 <= i - (DEPTH - 1) < count:
                second(i - (DEPTH - 1))
            if 0 <= i - 2 * (DEPTH - 1) < count:
                most = third(i - 2 * (DEPTH - 1), most)

        most = jnp.broadcast_to(level(jnp.max(most, axis=0, keepdims=True)), (8, LANES)).astype(I16)
        spare = lane_ids(8).astype(I16) == SUB + rows

        def share(t, carry):
            out[t, 0:8, :] = jnp.where(spare, most, out[t, 0:8, :])
            return carry

        lax.fori_loop(0, devices, share, 0, unroll=16)

    wide = 2 * LANES
    pl.run_scoped(
        products,
        *[pltpu.ACC(0)((2 * SUB, wide), F32) for _ in range(2 * DEPTH)],
        *[pltpu.ACC(1)((2 * per_row * rows, wide), F32) for _ in range(DEPTH)],
    )


def place_kernel(heads, owner, blocks, blank, clean, out, unit, acc):
    devices, rows, _ = blocks.shape
    aggs = acc.shape[0]
    tiles = acc.shape[2] // LANES
    lanes = lane_ids(8)
    bands = rows // 8

    def add(d, most):
        code = blocks[d].astype(F32)
        scale = jnp.exp2(code[:, rows : rows + 1] * 0.125) * (1.0 / TOP)
        sums = [jnp.zeros((rows, LANES), F32) for _ in range(tiles)]
        for q in range(4):
            start = heads[1 + q, d] * rows
            turned = pltpu.roll(code, (start - q * SUB + LANES) & (LANES - 1), 1)
            for m in range(tiles):
                at = (lanes + m * LANES) - start
                inside = at.astype(jnp.uint32) < rows
                inside = jnp.concatenate([inside] * bands, axis=0)
                sums[m] = jnp.where(inside, turned, sums[m])
        a = heads[0, d]
        for m in range(tiles):
            acc[a, :, m * LANES : (m + 1) * LANES] += sums[m] * scale
        return jnp.maximum(most, code[0:8])

    most = lax.fori_loop(0, devices, add, jnp.full((8, LANES), -8.0 * 1024, F32), unroll=128)
    most = jnp.broadcast_to(most[0:1, SUB + rows : SUB + rows + 1], (8, LANES))
    unit[...] = most
    inverse = jnp.exp2(FLOOR - most * 0.125)[0:1]
    rate = codes(devices)

    def send(a, carry):
        parts = []
        for m in range(tiles):
            value = acc[a, :, m * LANES : (m + 1) * LANES]
            size = jnp.log2(1.0 + jnp.abs(value) * inverse)
            parts.append(jnp.round(size * jnp.where(value < 0.0, -rate, rate)))
        out[owner[0, a]] = jnp.concatenate(parts, axis=0).astype(I16)
        return carry

    lax.fori_loop(0, aggs, send, 0, unroll=64)


def decode_kernel(unit, code, out, ready, sems):
    devices, rows, width = ready.shape
    parts = sems.shape[0]
    block = devices // parts
    delta = jnp.exp2(unit[0:1] * 0.125 - FLOOR)
    rate = 1.0 / codes(devices)

    def copy(g):
        here = pl.ds(g * block, block)
        return pltpu.make_async_copy(ready.at[here], out.at[here], sems.at[g])

    def step(g, carry):
        for j in range(block):
            d = g * block + j
            for m in range(width // LANES):
                x = code[d, rows * m : rows * (m + 1)].astype(F32)
                size = (jnp.exp2(jnp.abs(x) * rate) - 1.0) * jnp.where(x < 0.0, -delta, delta)
                ready[d, :, m * LANES : (m + 1) * LANES] = size
        copy(g).start()
        return carry

    lax.fori_loop(0, parts, step, 0)

    def finish(g, carry):
        copy(g).wait()
        return carry

    lax.fori_loop(0, parts, finish, 0)


def swap(x):
    return lax.all_to_all(x, AXES, split_axis=0, concat_axis=0, tiled=True)


def in_hbm(x):
    return pltpu.with_memory_space_constraint(x, pltpu.HBM)


def on_chip(x):
    return pltpu.with_memory_space_constraint(x, pltpu.VMEM)


def grant(mib):
    return pltpu.CompilerParams(vmem_limit_bytes=mib << 20)


def per_device(prolong, stiffness, request, col_slot, col_pos, coarse_owner):
    devices = lax.axis_size(AXES)
    aggs, rows, dof = prolong.shape
    per_row = stiffness.shape[1]
    width = MAXNB * rows
    smem = pl.BlockSpec(memory_space=pltpu.SMEM)
    vmem = pl.BlockSpec(memory_space=pltpu.VMEM)
    hbm = pl.BlockSpec(memory_space=pltpu.HBM)

    asking = jnp.concatenate([request[:, None], col_pos], axis=1)
    asked = swap(asking[:, None, :])[:, 0, :]

    depth = rows * (width // LANES)
    picked, heads, blank, clean = pl.pallas_call(
        pick_kernel,
        out_shape=(
            jax.ShapeDtypeStruct((devices, rows, dof), BF16),
            jax.ShapeDtypeStruct((8, devices), I32),
            jax.ShapeDtypeStruct((devices, depth, LANES), I16),
            jax.ShapeDtypeStruct((aggs, rows, width), F32),
        ),
        in_specs=[vmem, hbm, hbm, hbm, hbm],
        out_specs=(vmem, vmem, vmem, vmem),
        scratch_shapes=[
            pltpu.VMEM((aggs, rows, dof), BF16),
            pltpu.SMEM((8, devices), I32),
            pltpu.SemaphoreType.DMA((2,)),
        ],
        compiler_params=grant(8),
        name="pick",
    )(asked, in_hbm(prolong), in_hbm(stiffness), in_hbm(col_slot.T), in_hbm(coarse_owner.T))
    fetched = swap(picked)

    sent = pl.pallas_call(
        partial_kernel,
        out_shape=jax.ShapeDtypeStruct((devices, rows, LANES), I16),
        in_specs=[smem, vmem, vmem],
        out_specs=vmem,
        scratch_shapes=[pltpu.VMEM((devices, SUB, dof), BF16)],
        compiler_params=grant(16),
        name="partial",
    )(on_chip(col_slot.T), fetched, on_chip(stiffness))
    blocks = swap(sent)

    coarse, unit, _ = pl.pallas_call(
        place_kernel,
        out_shape=(
            jax.ShapeDtypeStruct((devices, depth, LANES), I16),
            jax.ShapeDtypeStruct((8, LANES), F32),
            jax.ShapeDtypeStruct((aggs, rows, width), F32),
        ),
        in_specs=[smem, smem, vmem, vmem, vmem],
        out_specs=(vmem, vmem, vmem),
        input_output_aliases={3: 0, 4: 2},
        compiler_params=grant(8),
        name="place",
    )(heads, on_chip(coarse_owner.T), blocks, blank, clean)
    arrived = swap(coarse)

    return pl.pallas_call(
        decode_kernel,
        out_shape=jax.ShapeDtypeStruct((devices, rows, width), F32),
        in_specs=[vmem, vmem],
        out_specs=hbm,
        scratch_shapes=[pltpu.VMEM((devices, rows, width), F32), pltpu.SemaphoreType.DMA((4,))],
        compiler_params=grant(16),
        name="decode",
    )(unit, arrived)


def solution(mesh):
    placed = (
        P(AXES, None, None),
        P(AXES, None, None, None),
        P(AXES),
        P(AXES, None),
        P(AXES, None),
        P(AXES, None),
    )
    return jax.shard_map(
        per_device, mesh=mesh, in_specs=placed, out_specs=P(AXES, None, None), check_vma=False
    )
```
